512 devices in a mesh: seq: 64 (over y, x, core), chan: 8 (over z).
Axes of the slice: x: 4, y: 8, z: 8, core: 2. Of those that a mesh axis runs over, the one named last changes fastest.
Arguments:
- x_in: bfloat16 [131072, 2048], P('seq', 'chan'), may hold values from -6 to 6
- gate_in: bfloat16 [131072, 2048], P('seq', 'chan'), may hold values from -70 to 70
- b_in: bfloat16 [131072, 64], P('seq'), may hold values from -0.75 to 0.75
- c_in: bfloat16 [131072, 64], P('seq'), may hold values from -6 to 6
- step_size: float32 [32, 131072], P('chan', 'seq'), may hold values from 0 to 1, as said below
- log_keep: float32 [32, 131072], P('chan', 'seq'), may hold values from -2 to 0
- skip_gain: float32 [32], P('chan'), may hold values from 0.5 to 1.5
- norm_gain: float32 [2048], P('chan'), may hold values from 0.25 to 1.75
Outputs:
- mixed: bfloat16 [131072, 2048], P('seq', 'chan')
The draws below stay inside these ranges and needn't reach their ends.
Inputs may be any that keep to these rules, and one draw needn't show every extreme that they name: `step_size`: positive.
All inputs are finite; a program needn't handle non-finite values.
Results may differ from the reference program's by a relative error of at most 0.005.
Values sent between devices are 32-bit elements; how exact they have to be, the bound alone decides.
No kernel may reach another device: no remote copies, remote signals or barrier semaphores. Data moves between devices by JAX's collectives and lax.ppermute only.
A program may use at most 64 MiB of HBM per device.

```python
import math
import jax
import jax.numpy as jnp
from jax import lax

CH = 2048
HEADDIM = 64
STATE = 64
BLOCK = 256
TOK_DEV = 2048
HEADS = 32
SEQUENCE_TOKENS = 131072


def decay_pieces(key):
    random_subkeys = jax.random.split(jax.random.fold_in(key, 17), 7)
    ranking = jax.random.permutation(random_subkeys[0], HEADS)
    slow_count = max(HEADS // 2, 1)
    is_slow = ranking < slow_count
    slow_rate = jnp.exp(jax.random.uniform(random_subkeys[1], (HEADS,), jnp.float32, math.log(0.2), math.log(0.5))) / SEQUENCE_TOKENS
    fast_rate = jnp.exp(jax.random.uniform(random_subkeys[2], (HEADS,), jnp.float32, math.log(0.02), math.log(0.05)))
    head_decay_rate = jnp.where(is_slow, slow_rate, fast_rate)
    token_multiplier = jnp.exp(jax.random.uniform(random_subkeys[3], (HEADS, SEQUENCE_TOKENS), jnp.float32, math.log(0.5), math.log(2.0)))
    device_multiplier = jnp.exp(jax.random.uniform(random_subkeys[4], (HEADS, SEQUENCE_TOKENS // TOK_DEV), jnp.float32, math.log(0.5), math.log(2.0)))
    device_multiplier = jnp.repeat(device_multiplier, TOK_DEV, axis=1)
    spike_position = jax.random.randint(random_subkeys[5], (2,), 0, SEQUENCE_TOKENS)
    spike_fraction = jax.random.uniform(random_subkeys[6], (2,), jnp.float32, 0.2, 0.5)
    token_positions = jnp.arange(SEQUENCE_TOKENS, dtype=jnp.int32)
    spike_amount = jnp.sum(jnp.where(token_positions[None, :] == spike_position[:, None], jnp.log(1.0 - spike_fraction)[:, None], 0.0), axis=0)
    return (head_decay_rate, head_decay_rate[:, None] * token_multiplier * device_multiplier, spike_amount)


def draw_log_keep(key, part):
    head_decay_rate, token_level, spike_amount = decay_pieces(key)
    return (spike_amount[None, :] - token_level).astype(jnp.float32)


def draw_step_size(key, part):
    head_decay_rate, token_level, spike_amount = decay_pieces(key)
    factor = jnp.exp(jax.random.uniform(jax.random.fold_in(key, 29), (HEADS, SEQUENCE_TOKENS), jnp.float32, math.log(0.5), math.log(2.0)))
    return (jnp.sqrt(2.0 * head_decay_rate)[:, None] * factor).astype(jnp.float32)


def draw_gate_in(key, part):
    random_subkeys = jax.random.split(jax.random.fold_in(key, 5), 2)
    column = jnp.arange(CH, dtype=jnp.float32) / max(CH - 1, 1)
    col_scale = jnp.sqrt(3.0) ** column * jnp.exp(jax.random.uniform(random_subkeys[0], (CH,), jnp.float32, 0.0, math.log(10.0)))
    noise_base = jnp.clip(jax.random.normal(random_subkeys[1], (SEQUENCE_TOKENS, CH), jnp.float32), -4.0, 4.0)
    return (noise_base * col_scale[None, :]).astype(jnp.bfloat16)


def steps_of(own_key, extent, shards, least, top_value):
    gain = 1.0
    for position, blocks in shards:
        steps = jax.random.uniform(jax.random.fold_in(jax.random.fold_in(own_key, 6), position), (blocks,), jnp.float32, least / len(shards), top_value / len(shards))
        gain = gain * jnp.repeat(jnp.exp(steps), extent[position] // blocks).reshape((-1,) + (1,) * (len(extent) - 1 - position))
    return gain


def noise(rng, dims, deviation, limit, cuts=(), kind=jnp.bfloat16):
    result = jax.random.normal(rng, dims, jnp.float32) * deviation
    if len(cuts) > 0:
        result = steps_of(rng, dims, cuts, -0.22, 0.18) * result
    return jnp.clip(result, min=-limit, max=limit).astype(kind)


def setup_inputs(seed: int = 0) -> dict:
    seeds = jax.random.split(jax.random.key(seed), 9)
    return {
        "x_in": noise(seeds[0], (SEQUENCE_TOKENS, CH), 1.0, 6.0, ((0, 64), (1, 8))),
        "gate_in": draw_gate_in(jax.random.fold_in(seeds[8], 71), 0),
        "b_in": noise(seeds[2], (SEQUENCE_TOKENS, STATE), STATE ** -0.5, 0.75, ((0, 64),)),
        "c_in": noise(seeds[3], (SEQUENCE_TOKENS, STATE), 1.0, 6.0, ((0, 64),)),
        "step_size": draw_step_size(jax.random.fold_in(seeds[8], 71), 0),
        "log_keep": draw_log_keep(jax.random.fold_in(seeds[8], 71), 0),
        "skip_gain": jnp.clip(0.5 + 1.0 * jax.random.uniform(seeds[6], (HEADS,), jnp.float32) ** steps_of(seeds[6], (HEADS,), ((0, 8),), -0.2, 0.2), 0.5, 1.5),
        "norm_gain": jnp.clip(1.0 + 0.15 * jax.random.normal(seeds[7], (CH,), jnp.float32), 0.25, 1.75),
    }


def reference(x_in, gate_in, b_in, c_in, step_size, log_keep, skip_gain, norm_gain):
    block_count = SEQUENCE_TOKENS // BLOCK
    x_blocks = x_in.reshape(block_count, BLOCK, HEADS, HEADDIM)
    b_blocks = b_in.reshape(block_count, BLOCK, STATE)
    c_blocks = c_in.reshape(block_count, BLOCK, STATE)
    keep_blocks = log_keep.reshape(HEADS, block_count, BLOCK).transpose(1, 0, 2)
    step_blocks = step_size.reshape(HEADS, block_count, BLOCK).transpose(1, 0, 2)
    row_index = lax.broadcasted_iota(jnp.int32, (BLOCK, BLOCK), 0)
    col_index = lax.broadcasted_iota(jnp.int32, (BLOCK, BLOCK), 1)
    causal = row_index >= col_index

    def advance(state_now, block_input):
        x_block, b_block, c_block, keep_block, step_block = block_input
        cum_keep = jnp.cumsum(keep_block, axis=1)
        block_total = cum_keep[:, -1]
        scores = jnp.dot(c_block, b_block.T, preferred_element_type=jnp.float32)
        log_gaps = cum_keep[:, :, None] - cum_keep[:, None, :]
        decays = jnp.where(causal[None], jnp.exp(jnp.where(causal[None], log_gaps, 0.0)), 0.0)
        weights = (scores[None] * decays * step_block[:, None, :]).astype(jnp.bfloat16)
        x_float = x_block.astype(jnp.float32)
        output = jnp.einsum('hts,shp->thp', weights.astype(jnp.float32), x_float)
        projected = jnp.einsum('tn,hpn->thp', c_block.astype(jnp.float32), state_now, precision=lax.Precision.HIGHEST)
        output = output + jnp.exp(cum_keep).T[:, :, None] * projected
        decayed_b = ((jnp.exp(block_total[:, None] - cum_keep) * step_block)[:, :, None] * b_block.astype(jnp.float32)[None]).astype(jnp.bfloat16)
        block_state = jnp.einsum('shp,hsn->hpn', x_float, decayed_b.astype(jnp.float32))
        next_state = jnp.exp(block_total)[:, None, None] * state_now + block_state
        return (next_state, output)
    initial = jnp.zeros((HEADS, HEADDIM, STATE), jnp.float32)
    _, outputs = lax.scan(advance, initial, (x_blocks, b_blocks, c_blocks, keep_blocks, step_blocks))
    recurrent = outputs + skip_gain[None, None, :, None] * x_blocks.astype(jnp.float32)
    recurrent = recurrent.reshape(SEQUENCE_TOKENS, CH)
    gated_out = recurrent * jax.nn.silu(gate_in.astype(jnp.float32))
    mean_square = lax.optimization_barrier(jnp.mean(gated_out * gated_out, axis=1))
    return (gated_out * lax.rsqrt(mean_square + 1e-05)[:, None] * norm_gain[None, :]).astype(jnp.bfloat16)
```

```python
import functools

import jax
import jax.numpy as jnp
from jax import lax
from jax.experimental import pallas as pl
from jax.experimental.pallas import tpu as pltpu
from jax.sharding import Mesh
from jax.sharding import PartitionSpec as P

CH = 2048
HEAD = 64
STATE = 64
SEQ = ("seq_0", "seq_1", "seq_2")
CUT = 128
EPSILON = 1e-05
LOG2E = 1.4426950408889634
MIB = 1024 * 1024

f32 = jnp.float32
bf16 = jnp.bfloat16
exact = functools.partial(
    jnp.dot, precision=lax.Precision.HIGHEST, preferred_element_type=f32
)


def dot(a, b):
    return jnp.dot(a, b, preferred_element_type=f32)


def dot_nt(a, b):
    return lax.dot_general(a, b, (((1,), (1,)), ((), ())), preferred_element_type=f32)


def dot_tn(a, b):
    return lax.dot_general(a, b, (((0,), (0,)), ((), ())), preferred_element_type=f32)


def iota(shape, axis):
    return lax.broadcasted_iota(jnp.int32, shape, axis)


def eye(rows, columns):
    return jnp.where(iota((rows, columns), 0) == iota((rows, columns), 1) % STATE, 1.0, 0.0)


def split3(v):
    high = v.astype(bf16).astype(f32)
    rest = v - high
    middle = rest.astype(bf16).astype(f32)
    return high, middle, rest - middle


def by_cut(ref):
    tokens = ref.shape[1]
    return jnp.concatenate([ref[:, k * CUT : (k + 1) * CUT] for k in range(tokens // CUT)], axis=0)


def two_heads(even, odd):
    return jnp.where(iota(even.shape, 1) < HEAD, even, odd)


def end_state_kernel(
    x_hbm, b_hbm, step_hbm, keep_hbm, out_ref,
    x_ref, b_ref, step_ref, keep_ref, factor, lhs, sems,
):
    copies = [
        pltpu.make_async_copy(source, target, sems.at[i])
        for i, (source, target) in enumerate(
            ((keep_hbm, keep_ref), (step_hbm, step_ref), (b_hbm, b_ref), (x_hbm, x_ref))
        )
    ]
    for copy in copies:
        copy.start()
    heads, tokens = step_ref.shape
    cuts = tokens // CUT
    row, col = iota((CUT, CUT), 0), iota((CUT, CUT), 1)
    copies[0].wait()
    keep = by_cut(keep_ref)
    after = exact(keep, jnp.where(row > col, 1.0, 0.0))
    total = exact(keep, jnp.ones((CUT, CUT), f32))
    count = heads * cuts
    row, col = iota((count, count), 0), iota((count, count), 1)
    same = row % heads == col % heads
    later = exact(jnp.where(same & (col // heads > row // heads), 1.0, 0.0), total)
    decay = jnp.exp(later[:heads] + total[:heads])
    lane = iota((1, CUT), 1) // (CUT // heads)
    decays = jnp.zeros((1, CUT), f32)
    for h in range(heads):
        decays = jnp.where(lane == h, decay[h : h + 1], decays)
    copies[1].wait()
    factor[...] = jnp.exp(after + later) * by_cut(step_ref)
    copies[2].wait()
    for k in range(cuts):
        part = b_ref[:, k * CUT : (k + 1) * CUT].astype(f32)
        for h in range(heads):
            scaled = part * factor[k * heads + h : k * heads + h + 1, :]
            lhs[h * STATE : (h + 1) * STATE, k * CUT : (k + 1) * CUT] = scaled.astype(bf16)
    copies[3].wait()
    pairs = heads // 2
    for pair in range(pairs):
        lanes = slice(pair * CUT, (pair + 1) * CUT)
        both = dot(lhs[pair * 2 * STATE : (pair + 1) * 2 * STATE, :], x_ref[:, lanes])
        out_ref[:, 0, lanes] = two_heads(both[:STATE], both[STATE:])
    out_ref[:, 0, pairs * CUT :] = jnp.broadcast_to(decays, (STATE, CUT))


def scan_kernel(heads, got_ref, _, out_ref, state_ref, decay_ref):
    count = got_ref.shape[0]
    width = heads * HEAD
    state_ref[...] = got_ref[:, 0, :width]
    row, col = iota((CUT, width), 0), iota((CUT, width), 1)
    spread = jnp.where(row == col // HEAD * (CUT // heads), 1.0, 0.0)
    decay_ref[...] = exact(got_ref[:, 0, width:], spread)
    state = jnp.zeros((1, width), f32)
    for k in range(count):
        out_ref[k] = state
        state = decay_ref[k : k + 1, :] * state + state_ref[k : k + 1, :]


def local_kernel(
    skip_ref, x_hbm, gate_hbm, b_hbm, c_hbm, step_hbm, keep_hbm,
    base_ref, carry_ref, flag_ref,
    x_ref, gate_ref, b_ref, c_ref, step_ref, keep_ref,
    left, offset, factor, decays, starts, state, sems, x_sems, gate_sems,
):
    copies = [
        pltpu.make_async_copy(source, target, sems.at[i])
        for i, (source, target) in enumerate(
            ((keep_hbm, keep_ref), (step_hbm, step_ref), (b_hbm, b_ref), (c_hbm, c_ref))
        )
    ]
    for copy in copies:
        copy.start()

    def tiles(k):
        at = pl.ds(pl.multiple_of(k * CUT, CUT), CUT)
        return (
            pltpu.make_async_copy(x_hbm.at[at], x_ref.at[at], x_sems.at[k]),
            pltpu.make_async_copy(gate_hbm.at[at], gate_ref.at[at], gate_sems.at[k]),
        )

    def start(k, _):
        for copy in tiles(k):
            copy.start()
        return 0

    lax.fori_loop(0, x_hbm.shape[0] // CUT, start, 0)
    flag_ref[...] = jnp.zeros_like(flag_ref)
    for copy in copies:
        copy.wait()
    heads, tokens = step_ref.shape
    channels = x_ref.shape[1]
    cuts = tokens // CUT
    count = heads * cuts
    keep = by_cut(keep_ref)
    step = by_cut(step_ref)
    row, col = iota((CUT, CUT), 0), iota((CUT, CUT), 1)
    upto = exact(keep, jnp.where(row <= col, 1.0, 0.0)) * LOG2E
    after = exact(keep, jnp.where(row > col, 1.0, 0.0))
    total = exact(keep, jnp.ones((CUT, CUT), f32))
    big_row, big_col = iota((count, count), 0), iota((count, count), 1)
    same = big_row % heads == big_col % heads
    before = exact(jnp.where(same & (big_col // heads < big_row // heads), 1.0, 0.0), total)
    factor[...] = jnp.exp(after) * step
    decays[...] = jnp.exp(total)
    starts[...] = jnp.exp(before)
    pieces = split3(upto)
    minus = split3(jnp.log2(jnp.maximum(step, 1e-37)) - upto)
    for k in range(cuts):
        at = slice(k * heads, (k + 1) * heads)
        left[k] = jnp.concatenate([piece[at] for piece in pieces] + [jnp.ones((4, CUT), f32)], axis=0)
        rows = [
            jnp.concatenate([piece[k * heads + h : k * heads + h + 1] for h in range(heads)], axis=1)
            for piece in minus
        ]
        offset[k] = jnp.concatenate(rows + [jnp.zeros((1, heads * CUT), f32)], axis=0)
    state[...] = jnp.zeros_like(state)
    double = eye(STATE, 2 * STATE).astype(bf16)
    pick_row, pick_col = iota((12, heads * CUT), 0), iota((12, heads * CUT), 1)
    pick = jnp.where(pick_row % heads == pick_col // CUT, 1.0, 0.0)
    wide_row, wide_col = iota((16, channels), 0), iota((16, channels), 1)
    wide = jnp.where((wide_row % heads == wide_col // HEAD) & (wide_row < 12), 1.0, 0.0)
    lane_head = iota((1, channels), 1) // HEAD
    only = [jnp.where(lane_head == h, 1.0, 0.0).astype(bf16) for h in range(heads)]
    skip = jnp.zeros((1, channels), f32)
    for h in range(heads):
        skip = jnp.where(lane_head == h, skip_ref[h], skip)

    def per_channel(ref, first):
        wide_rows = [
            two_heads(ref[pl.ds(first + 2 * p, 1), :], ref[pl.ds(first + 2 * p + 1, 1), :])
            for p in range(heads // 2)
        ]
        return jnp.concatenate(wide_rows, axis=1)

    def one_cut(k, _):
        at = pl.ds(pl.multiple_of(k * CUT, CUT), CUT)
        first = k * heads
        for copy in tiles(k):
            copy.wait()
        x = x_ref[at, :]
        b = b_ref[:, at]
        twice = dot_tn(c_ref[:, at], double).astype(bf16)
        lhs = jnp.transpose(left[k]).astype(bf16)
        rhs = jnp.concatenate([jnp.concatenate([pick, offset[k]], axis=0), wide], axis=1).astype(bf16)
        gaps = dot(lhs, rhs)
        scores = jnp.where(row >= col, dot(twice[:, :STATE], b), 0.0)
        weights = [
            (scores * jnp.exp2(jnp.minimum(gaps[:, h * CUT : (h + 1) * CUT], 0.0))).astype(bf16)
            for h in range(heads)
        ]
        inside = dot(
            jnp.concatenate(weights, axis=1), jnp.concatenate([x * mask for mask in only], axis=0)
        )
        now = state[...]
        high = now.astype(bf16)
        low = (now - high.astype(f32)).astype(bf16)
        earlier = dot(twice, jnp.concatenate([high, low], axis=0))
        growth = jnp.exp2(gaps[:, heads * CUT :])
        gate = gate_ref[at, :].astype(f32)
        gate = gate / (1.0 + jnp.exp(-gate))
        base_ref[at, :] = (inside + growth * earlier + skip * x.astype(f32)) * gate
        carry_ref[at, :] = (growth * per_channel(starts, first) * gate).astype(bf16)
        b_turned = b.astype(f32)
        ends = []
        for pair in range(heads // 2):
            scaled = [
                b_turned * factor[pl.ds(first + 2 * pair + i, 1), :] for i in range(2)
            ]
            both = dot(
                jnp.concatenate(scaled, axis=0).astype(bf16), x[:, pair * CUT : (pair + 1) * CUT]
            )
            ends.append(two_heads(both[:STATE], both[STATE:]))
        state[...] = per_channel(decays, first) * now + jnp.concatenate(ends, axis=1)
        return 0

    lax.fori_loop(0, cuts, one_cut, 0)


def gate_kernel(got_ref, c_ref, base_ref, carry_ref, gated_ref, squares_ref):
    peers = squares_ref.shape[0]
    tokens = base_ref.shape[0]
    now = got_ref[:, 0, :]
    high = now.astype(bf16)
    low = (now - high.astype(f32)).astype(bf16)
    both = jnp.concatenate([high, low], axis=0)
    ones = jnp.ones((8, 2 * CUT), bf16)
    size = 2 * CUT
    for k in range(tokens // size):
        at = slice(k * size, (k + 1) * size)
        c = c_ref[:, at]
        added = dot_tn(jnp.concatenate([c, c], axis=0), both)
        gated = base_ref[at, :] + carry_ref[at, :].astype(f32) * added
        gated_ref[at, :] = gated
        square = gated * gated
        square = square[:, :CUT] + square[:, CUT:]
        high = square.astype(bf16)
        low = (square - high.astype(f32)).astype(bf16)
        summed = dot_nt(ones, jnp.concatenate([high, low], axis=1))
        for peer in range(peers):
            for half in range(2):
                squares_ref[peer, 2 * k + half : 2 * k + half + 1, :] = summed[
                    :1, half * CUT : (half + 1) * CUT
                ]


def norm_kernel(got_ref, gain_ref, gated_ref, out_hbm, out_ref, sems):
    peers = got_ref.shape[0]
    cuts = got_ref.shape[1]
    summed = got_ref[0]
    for peer in range(1, peers):
        summed = summed + got_ref[peer]
    pieces = split3(lax.rsqrt(summed / CH + EPSILON))
    gain = gain_ref[...]
    ones = jnp.where(iota((8, gain.shape[1]), 0) < 3, 1.0, 0.0).astype(bf16)
    copies = []
    for k in range(cuts):
        at = slice(k * CUT, (k + 1) * CUT)
        rows = [piece[k : k + 1] for piece in pieces] + [jnp.zeros((5, CUT), f32)]
        factor = dot(jnp.transpose(jnp.concatenate(rows, axis=0)).astype(bf16), ones)
        out_ref[at, :] = (gated_ref[at, :] * factor * gain).astype(bf16)
        if k % 4 == 3:
            four = pl.ds((k - 3) * CUT, 4 * CUT)
            copy = pltpu.make_async_copy(out_ref.at[four], out_hbm.at[four], sems.at[k // 4])
            copy.start()
            copies.append(copy)
    for copy in copies:
        copy.wait()


VMEM = pl.BlockSpec(memory_space=pltpu.VMEM)
SMEM = pl.BlockSpec(memory_space=pltpu.SMEM)
HBM = pl.BlockSpec(memory_space=pltpu.HBM)


def call(kernel, out_shape, in_specs, scratch=(), out_specs=None, flops=1000000):
    return pl.pallas_call(
        kernel,
        out_shape=out_shape,
        in_specs=in_specs,
        out_specs=out_specs or jax.tree.map(lambda _: VMEM, out_shape),
        scratch_shapes=list(scratch),
        cost_estimate=pl.CostEstimate(flops=flops, bytes_accessed=4 * MIB, transcendentals=0),
        compiler_params=pltpu.CompilerParams(vmem_limit_bytes=16 * MIB),
    )


def per_device(x_in, gate_in, b_in, c_in, step_size, log_keep, skip_gain, norm_gain):
    tokens, channels = x_in.shape
    heads = step_size.shape[0]
    cuts = tokens // CUT
    shape = jax.ShapeDtypeStruct
    dma = pltpu.SemaphoreType.DMA
    b_turned, c_turned = b_in.T, c_in.T
    x_in, gate_in, b_turned, c_far, step_size, log_keep, skip_gain = (
        pltpu.with_memory_space_constraint(v, pltpu.HBM)
        for v in (x_in, gate_in, b_turned, c_turned, step_size, log_keep, skip_gain)
    )
    rows = pltpu.VMEM((heads * cuts, CUT), f32)
    wide = pltpu.VMEM((tokens, channels), bf16)
    turned = pltpu.VMEM((STATE, tokens), bf16)
    small = pltpu.VMEM((heads, tokens), f32)
    message = call(
        end_state_kernel,
        shape((STATE, 1, channels + CUT), f32),
        [HBM] * 4,
        [wide, turned, small, small, rows, pltpu.VMEM((heads * STATE, tokens), bf16), dma((4,))],
        flops=2 * tokens * STATE * channels,
    )(x_in, b_turned, step_size, log_keep)
    got = lax.all_to_all(message, SEQ, 0, 0, tiled=True)
    base, carry, flag = call(
        local_kernel,
        (shape((tokens, channels), f32), shape((tokens, channels), bf16), shape((8, CUT), f32)),
        [SMEM] + [HBM] * 6,
        [wide, wide, turned, turned, small, small]
        + [pltpu.VMEM((cuts, 16, CUT), f32), pltpu.VMEM((cuts, 4, heads * CUT), f32)]
        + [rows] * 3
        + [pltpu.VMEM((STATE, channels), f32), dma((4,)), dma((cuts,)), dma((cuts,))],
        flops=int(5e9),
    )(skip_gain, x_in, gate_in, b_turned, c_far, step_size, log_keep)
    row = pltpu.VMEM((STATE, channels), f32)
    before = call(
        functools.partial(scan_kernel, heads),
        shape((STATE, 1, channels), f32),
        [VMEM] * 2,
        [row, row],
    )(got, flag)
    entering = lax.all_to_all(before, SEQ, 0, 0, tiled=True)
    peers = lax.axis_size("chan")
    gated, squares = call(
        gate_kernel,
        (shape((tokens, channels), f32), shape((peers, cuts, CUT), f32)),
        [VMEM] * 4,
        flops=2 * tokens * STATE * channels,
    )(entering, c_turned, base, carry)
    summed = lax.all_to_all(squares, "chan", 0, 0, tiled=True)
    return call(
        norm_kernel,
        shape((tokens, channels), bf16),
        [VMEM] * 3,
        [wide, dma((4,))],
        out_specs=HBM,
    )(summed, norm_gain.reshape(1, channels), gated)


def solution(mesh):
    chan = mesh.shape["chan"]
    split = Mesh(mesh.devices.reshape(8, 4, 2, chan), (*SEQ, "chan"))
    placed = (
        P(SEQ, "chan"),
        P(SEQ, "chan"),
        P(SEQ, None),
        P(SEQ, None),
        P("chan", SEQ),
        P("chan", SEQ),
        P("chan"),
        P("chan"),
    )
    return jax.shard_map(
        per_device, mesh=split, in_specs=placed, out_specs=P(SEQ, "chan"), check_vma=False
    )
```

```python
import functools

import jax
import jax.numpy as jnp
from jax import lax
from jax.experimental import pallas as pl
from jax.experimental.pallas import tpu as pltpu
from jax.sharding import Mesh
from jax.sharding import PartitionSpec as P

CH = 2048
HEAD = 64
STATE = 64
SEQ = ("seq_0", "seq_1", "seq_2")
CUT = 128
EPSILON = 1e-05
LOG2E = 1.4426950408889634
MIB = 1024 * 1024
UNROLL = 4

f32 = jnp.float32
bf16 = jnp.bfloat16
exact = functools.partial(
    jnp.dot, precision=lax.Precision.HIGHEST, preferred_element_type=f32
)


def dot(a, b):
    return jnp.dot(a, b, preferred_element_type=f32)


def dot_nt(a, b):
    return lax.dot_general(a, b, (((1,), (1,)), ((), ())), preferred_element_type=f32)


def dot_tn(a, b):
    return lax.dot_general(a, b, (((0,), (0,)), ((), ())), preferred_element_type=f32)


def iota(shape, axis):
    return lax.broadcasted_iota(jnp.int32, shape, axis)


def split3(v):
    high = v.astype(bf16).astype(f32)
    rest = v - high
    middle = rest.astype(bf16).astype(f32)
    return high, middle, rest - middle


def sum_of_pieces(v, zeros_and_ones):
    ones = zeros_and_ones.astype(bf16)
    high, middle, low = (dot(piece.astype(bf16), ones) for piece in split3(v))
    return high + (middle + low)


def by_cut(ref):
    tokens = ref.shape[1]
    return jnp.concatenate([ref[:, k * CUT : (k + 1) * CUT] for k in range(tokens // CUT)], axis=0)


def two_heads(even, odd):
    return jnp.where(iota(even.shape, 1) < HEAD, even, odd)


def end_state_kernel(
    x_hbm, b_hbm, c_hbm, step_hbm, keep_hbm,
    out_ref, x_ref, b_ref, c_ref, step_ref, keep_ref,
    x_rest, factor, lhs, sems,
):
    half = x_ref.shape[0]
    copies = [
        pltpu.make_async_copy(source, target, sems.at[i])
        for i, (source, target) in enumerate(
            (
                (keep_hbm, keep_ref),
                (step_hbm, step_ref),
                (b_hbm, b_ref),
                (x_hbm.at[pl.ds(0, half)], x_ref),
                (x_hbm.at[pl.ds(half, half)], x_rest),
                (c_hbm, c_ref),
            )
        )
    ]
    for copy in copies:
        copy.start()
    heads, tokens = step_ref.shape
    cuts = tokens // CUT
    row, col = iota((CUT, 2 * CUT), 0), iota((CUT, 2 * CUT), 1)
    kept = jnp.where((row > col) | (col >= CUT), 1.0, 0.0)
    copies[0].wait()
    sums = sum_of_pieces(by_cut(keep_ref), kept)
    after, total = sums[:, :CUT], sums[:, CUT:]
    count = heads * cuts
    row, col = iota((count, count), 0), iota((count, count), 1)
    same = row % heads == col % heads
    later = exact(jnp.where(same & (col // heads > row // heads), 1.0, 0.0), total)
    decay = jnp.exp(later[:heads] + total[:heads])
    lane = iota((1, CUT), 1) // (CUT // heads)
    decays = jnp.zeros((1, CUT), f32)
    for h in range(heads):
        decays = jnp.where(lane == h, decay[h : h + 1], decays)
    copies[1].wait()
    factor[...] = jnp.exp(after + later) * by_cut(step_ref)
    copies[2].wait()
    for k in range(cuts):
        part = b_ref[:, k * CUT : (k + 1) * CUT].astype(f32)
        for h in range(heads):
            scaled = part * factor[k * heads + h : k * heads + h + 1, :]
            lhs[h * STATE : (h + 1) * STATE, k * CUT : (k + 1) * CUT] = scaled.astype(bf16)
    copies[3].wait()
    copies[4].wait()
    pairs = heads // 2
    for pair in range(pairs):
        lanes = slice(pair * CUT, (pair + 1) * CUT)
        rows = slice(pair * 2 * STATE, (pair + 1) * 2 * STATE)
        both = dot(lhs[rows, :half], x_ref[:, lanes]) + dot(lhs[rows, half:], x_rest[:, lanes])
        out_ref[:, 0, lanes] = two_heads(both[:STATE], both[STATE:])
    out_ref[:, 0, pairs * CUT :] = jnp.broadcast_to(decays, (STATE, CUT))
    copies[5].wait()


def scan_kernel(heads, got_ref, _, out_ref, flag_ref, state_ref, decay_ref):
    flag_ref[...] = jnp.zeros_like(flag_ref)
    count = got_ref.shape[0]
    width = heads * HEAD
    state_ref[...] = got_ref[:, 0, :width]
    row, col = iota((CUT, width), 0), iota((CUT, width), 1)
    spread = jnp.where(row == col // HEAD * (CUT // heads), 1.0, 0.0)
    decay_ref[...] = exact(got_ref[:, 0, width:], spread)
    state = jnp.zeros((1, width), f32)
    for k in range(count):
        out_ref[k] = state
        state = decay_ref[k : k + 1, :] * state + state_ref[k : k + 1, :]


def tile_copies(skipped, pairs, sems):
    def copies(k):
        source = pl.ds(pl.multiple_of((skipped + k) * CUT, CUT), CUT)
        at = pl.ds(pl.multiple_of(k * CUT, CUT), CUT)
        return [
            pltpu.make_async_copy(far.at[source], near.at[at], sems.at[i, k])
            for i, (far, near) in enumerate(pairs)
        ]

    def wait(k):
        for copy in copies(k):
            copy.wait()

    for k in range(pairs[0][1].shape[0] // CUT):
        for copy in copies(k):
            copy.start()
    return wait


def early_kernel(
    skip_ref, x_ref, b_ref, c_ref, step_ref, keep_ref, gate_hbm,
    base_ref, carry_ref, state_out, gate_ref, *rest,
):
    *scratch, state, sems = rest
    wait = tile_copies(0, [(gate_hbm, gate_ref)], sems)
    state[...] = jnp.zeros_like(state)
    cut_by_cut(
        0, skip_ref, x_ref, gate_ref, b_ref, c_ref, step_ref, keep_ref, base_ref, carry_ref,
        *scratch, state, wait, lambda: None,
    )
    state_out[...] = state[...]


def late_kernel(
    flag_ref, state_in, skip_ref, x_hbm, b_hbm, c_hbm, step_hbm, keep_hbm, gate_hbm,
    base_ref, carry_ref, gate_ref, *rest,
):
    *scratch, state, sems, x_ref, b_ref, c_ref, step_ref, keep_ref, more_sems = rest
    copies = [
        pltpu.make_async_copy(far, near, more_sems.at[i])
        for i, (far, near) in enumerate(
            ((keep_hbm, keep_ref), (step_hbm, step_ref), (b_hbm, b_ref), (c_hbm, c_ref))
        )
    ]
    for copy in copies:
        copy.start()
    skipped = x_ref.shape[0] // CUT
    wait = tile_copies(skipped, [(x_hbm, x_ref), (gate_hbm, gate_ref)], sems)
    state[...] = state_in[...]
    copies[0].wait()
    copies[1].wait()

    def wait_both():
        copies[2].wait()
        copies[3].wait()

    cut_by_cut(
        skipped, skip_ref, x_ref, gate_ref, b_ref, c_ref, step_ref, keep_ref,
        base_ref, carry_ref, *scratch, state, wait, wait_both,
    )


def cut_by_cut(
    skipped, skip_ref, x_ref, gate_ref, b_ref, c_ref, step_ref, keep_ref, base_ref, carry_ref,
    left, offset, factor, decays, starts, state, wait_tile, wait_rest,
):
    heads, tokens = step_ref.shape
    cuts = tokens // CUT
    mine = x_ref.shape[0] // CUT
    count = heads * cuts
    step = by_cut(step_ref)
    row, col = iota((CUT, 3 * CUT), 0), iota((CUT, 3 * CUT), 1)
    kind = col // CUT
    kept = (kind == 2) | ((kind == 0) & (row <= col)) | ((kind == 1) & (row > col - CUT))
    sums = sum_of_pieces(by_cut(keep_ref), jnp.where(kept, 1.0, 0.0))
    upto, after, total = (sums[:, i * CUT : (i + 1) * CUT] for i in range(3))
    upto = upto * LOG2E
    row, col = iota((count, count), 0), iota((count, count), 1)
    earlier_cut = (row % heads == col % heads) & (col // heads < row // heads)
    factor[...] = jnp.exp(after) * step
    decays[...] = jnp.exp(total)
    starts[...] = jnp.exp(exact(jnp.where(earlier_cut, 1.0, 0.0), total))
    offset[...] = jnp.log2(jnp.maximum(step, 1e-37)) - upto
    for k in range(mine):
        rows = upto[(skipped + k) * heads : (skipped + k + 1) * heads]
        left[k] = jnp.concatenate([rows, jnp.zeros((8 - heads, CUT), f32)], axis=0)
    row, col = iota((CUT, CUT), 0), iota((CUT, CUT), 1)
    causal = row >= col
    low_lanes = jnp.where(iota((1, CUT), 1) < HEAD, 1.0, 0.0)
    only = [low_lanes.astype(bf16), (1.0 - low_lanes).astype(bf16)]

    def one_cut(k, _):
        at = pl.ds(pl.multiple_of(k * CUT, CUT), CUT)
        far = pl.ds(pl.multiple_of((skipped + k) * CUT, CUT), CUT)
        first = (skipped + k) * heads
        wait_tile(k)
        b = b_ref[:, far]
        c = jnp.transpose(c_ref[:, far])
        growths = jnp.transpose(left[k])
        growths = [jnp.broadcast_to(growths[:, h : h + 1], (CUT, CUT)) for h in range(heads)]
        scores = jnp.where(causal, dot(c, b), 0.0)
        b_turned = b.astype(f32)
        now = state[...]
        high = now.astype(bf16)
        low = (now - high.astype(f32)).astype(bf16)
        earlier = dot(jnp.concatenate([c, c], axis=1), jnp.concatenate([high, low], axis=0))
        for pair in range(heads // 2):
            lanes = slice(pair * CUT, (pair + 1) * CUT)
            x = x_ref[at, lanes]
            weights = []
            for h in range(2 * pair, 2 * pair + 2):
                gaps = growths[h] + offset[pl.ds(first + h, 1), :]
                weights.append((scores * jnp.exp2(jnp.minimum(gaps, 0.0))).astype(bf16))
            inside = dot(
                jnp.concatenate(weights, axis=1), jnp.concatenate([x * mask for mask in only], axis=0)
            )
            growth = jnp.exp2(two_heads(growths[2 * pair], growths[2 * pair + 1]))
            gate = gate_ref[at, lanes].astype(f32)
            gate = gate * pl.reciprocal(1.0 + jnp.exp(-gate))
            skip = two_heads(
                jnp.full((1, CUT), skip_ref[2 * pair]), jnp.full((1, CUT), skip_ref[2 * pair + 1])
            )
            base_ref[at, lanes] = (inside + growth * earlier[:, lanes] + skip * x.astype(f32)) * gate

            def per_channel(ref):
                even = first + 2 * pair
                return two_heads(ref[pl.ds(even, 1), :], ref[pl.ds(even + 1, 1), :])

            carry_ref[at, lanes] = (growth * per_channel(starts) * gate).astype(bf16)
            scaled = [b_turned * factor[pl.ds(first + 2 * pair + i, 1), :] for i in range(2)]
            both = dot(jnp.concatenate(scaled, axis=0).astype(bf16), x)
            state[:, lanes] = per_channel(decays) * now[:, lanes] + two_heads(both[:STATE], both[STATE:])
        return 0

    wait_rest()
    lax.fori_loop(0, mine, one_cut, 0, unroll=UNROLL)


def gate_kernel(got_ref, c_ref, *refs):
    *parts, gated_ref, squares_ref = refs
    peers = squares_ref.shape[0]
    tokens = gated_ref.shape[0]
    now = got_ref[:, 0, :]
    high = now.astype(bf16)
    low = (now - high.astype(f32)).astype(bf16)
    both = jnp.concatenate([high, low], axis=0)
    ones = jnp.ones((8, 2 * CUT), bf16)
    size = 2 * CUT
    half_tokens = tokens // (len(parts) // 2)
    for k in range(tokens // size):
        at = slice(k * size, (k + 1) * size)
        c = c_ref[:, at]
        added = dot_tn(jnp.concatenate([c, c], axis=0), both)
        first = k * size
        base_ref, carry_ref = parts[2 * (first // half_tokens) : 2 * (first // half_tokens) + 2]
        here = slice(first % half_tokens, first % half_tokens + size)
        gated = base_ref[here, :] + carry_ref[here, :].astype(f32) * added
        gated_ref[at, :] = gated
        square = gated * gated
        square = square[:, :CUT] + square[:, CUT:]
        high = square.astype(bf16)
        low = (square - high.astype(f32)).astype(bf16)
        summed = dot_nt(ones, jnp.concatenate([high, low], axis=1))
        for peer in range(peers):
            for half in range(2):
                squares_ref[peer, 2 * k + half : 2 * k + half + 1, :] = summed[
                    :1, half * CUT : (half + 1) * CUT
                ]


def norm_kernel(got_ref, gain_ref, gated_ref, out_hbm, out_ref, sems):
    peers = got_ref.shape[0]
    cuts = got_ref.shape[1]
    summed = got_ref[0]
    for peer in range(1, peers):
        summed = summed + got_ref[peer]
    pieces = split3(lax.rsqrt(summed / CH + EPSILON))
    gain = gain_ref[...]
    ones = jnp.where(iota((8, gain.shape[1]), 0) < 3, 1.0, 0.0).astype(bf16)
    copies = []
    for k in range(cuts):
        at = slice(k * CUT, (k + 1) * CUT)
        rows = [piece[k : k + 1] for piece in pieces] + [jnp.zeros((5, CUT), f32)]
        factor = dot(jnp.transpose(jnp.concatenate(rows, axis=0)).astype(bf16), ones)
        out_ref[at, :] = (gated_ref[at, :] * factor * gain).astype(bf16)
        if k % 4 == 3:
            four = pl.ds((k - 3) * CUT, 4 * CUT)
            copy = pltpu.make_async_copy(out_ref.at[four], out_hbm.at[four], sems.at[k // 4])
            copy.start()
            copies.append(copy)
    for copy in copies:
        copy.wait()


VMEM = pl.BlockSpec(memory_space=pltpu.VMEM)
SMEM = pl.BlockSpec(memory_space=pltpu.SMEM)
HBM = pl.BlockSpec(memory_space=pltpu.HBM)


def call(kernel, out_shape, in_specs, scratch=(), out_specs=None, flops=1000000):
    return pl.pallas_call(
        kernel,
        out_shape=out_shape,
        in_specs=in_specs,
        out_specs=out_specs or jax.tree.map(lambda _: VMEM, out_shape),
        scratch_shapes=list(scratch),
        cost_estimate=pl.CostEstimate(flops=flops, bytes_accessed=4 * MIB, transcendentals=0),
        compiler_params=pltpu.CompilerParams(vmem_limit_bytes=16 * MIB),
    )


def per_device(x_in, gate_in, b_in, c_in, step_size, log_keep, skip_gain, norm_gain):
    tokens, channels = x_in.shape
    heads = step_size.shape[0]
    cuts = tokens // CUT
    shape = jax.ShapeDtypeStruct
    dma = pltpu.SemaphoreType.DMA
    b_turned, c_turned = b_in.T, c_in.T
    x_in, gate_in, b_turned, c_far, step_size, log_keep, skip_gain = (
        pltpu.with_memory_space_constraint(v, pltpu.HBM)
        for v in (x_in, gate_in, b_turned, c_turned, step_size, log_keep, skip_gain)
    )
    rows = pltpu.VMEM((heads * cuts, CUT), f32)
    half = tokens // 2
    row = pltpu.VMEM((STATE, channels), f32)
    part = shape((half, channels), bf16)
    turned = shape((STATE, tokens), bf16)
    per_head = shape((heads, tokens), f32)
    near_shapes = (turned, turned, per_head, per_head)
    local_shapes = (shape((half, channels), f32), part)
    half_wide = pltpu.VMEM((half, channels), bf16)
    local_scratch = [
        half_wide,
        pltpu.VMEM((cuts // 2, 8, CUT), f32),
        rows,
        rows, rows, rows, row,
    ]
    message, x_near, *near = call(
        end_state_kernel,
        (shape((STATE, 1, channels + CUT), f32), part, *near_shapes),
        [HBM] * 5,
        [half_wide, rows, pltpu.VMEM((heads * STATE, tokens), bf16), dma((6,))],
        flops=2 * tokens * STATE * channels,
    )(x_in, b_turned, c_far, step_size, log_keep)
    got = lax.all_to_all(message, SEQ, 0, 0, tiled=True)
    base_0, carry_0, state = call(
        early_kernel,
        (*local_shapes, shape((STATE, channels), f32)),
        [SMEM] + [VMEM] * 5 + [HBM],
        [*local_scratch, dma((1, cuts // 2))],
        flops=int(5e9),
    )(skip_gain, x_near, *near, gate_in)
    before, flag = call(
        functools.partial(scan_kernel, heads),
        (shape((STATE, 1, channels), f32), shape((8, CUT), f32)),
        [VMEM] * 2,
        [row, row],
    )(got, state)
    entering = lax.all_to_all(before, SEQ, 0, 0, tiled=True)
    base_1, carry_1 = call(
        late_kernel,
        local_shapes,
        [VMEM] * 2 + [SMEM] + [HBM] * 6,
        [
            *local_scratch, dma((2, cuts // 2)), half_wide,
            *(pltpu.VMEM(v.shape, v.dtype) for v in near_shapes), dma((4,)),
        ],
        flops=int(5e9),
    )(flag, state, skip_gain, x_in, b_turned, c_far, step_size, log_keep, gate_in)
    peers = lax.axis_size("chan")
    gated, squares = call(
        gate_kernel,
        (shape((tokens, channels), f32), shape((peers, cuts, CUT), f32)),
        [VMEM] * 6,
        flops=2 * tokens * STATE * channels,
    )(entering, c_turned, base_0, carry_0, base_1, carry_1)
    summed = lax.all_to_all(squares, "chan", 0, 0, tiled=True)
    return call(
        norm_kernel,
        shape((tokens, channels), bf16),
        [VMEM] * 3,
        [pltpu.VMEM((tokens, channels), bf16), dma((4,))],
        out_specs=HBM,
    )(summed, norm_gain.reshape(1, channels), gated)


def solution(mesh):
    chan = mesh.shape["chan"]
    split = Mesh(mesh.devices.reshape(8, 4, 2, chan), (*SEQ, "chan"))
    placed = (
        P(SEQ, "chan"),
        P(SEQ, "chan"),
        P(SEQ, None),
        P(SEQ, None),
        P("chan", SEQ),
        P("chan", SEQ),
        P("chan"),
        P("chan"),
    )
    return jax.shard_map(
        per_device, mesh=split, in_specs=placed, out_specs=P(SEQ, "chan"), check_vma=False
    )
```

```python
import functools

import jax
import jax.numpy as jnp
from jax import lax
from jax.experimental import pallas as pl
from jax.experimental.pallas import tpu as pltpu
from jax.sharding import PartitionSpec as P

CH = 2048
HEAD = 64
STATE = 64
SEQ = "seq"
CUT = 128
EPSILON = 1e-05
LOG2E = 1.4426950408889634
MIB = 1024 * 1024
UNROLL = 4
FIRST = {"seq": 45, "chan": 5}

f32 = jnp.float32
bf16 = jnp.bfloat16
exact = functools.partial(
    jnp.dot, precision=lax.Precision.HIGHEST, preferred_element_type=f32
)


def dot(a, b):
    return jnp.dot(a, b, preferred_element_type=f32)


def dot_nt(a, b):
    return lax.dot_general(a, b, (((1,), (1,)), ((), ())), preferred_element_type=f32)


def dot_tn(a, b):
    return lax.dot_general(a, b, (((0,), (0,)), ((), ())), preferred_element_type=f32)


def iota(shape, axis):
    return lax.broadcasted_iota(jnp.int32, shape, axis)


def split3(v):
    high = v.astype(bf16).astype(f32)
    rest = v - high
    middle = rest.astype(bf16).astype(f32)
    return high, middle, rest - middle


def sum_of_pieces(v, zeros_and_ones):
    ones = zeros_and_ones.astype(bf16)
    high, middle, low = (dot(piece.astype(bf16), ones) for piece in split3(v))
    return high + (middle + low)


def by_cut(ref):
    tokens = ref.shape[1]
    return jnp.concatenate([ref[:, k * CUT : (k + 1) * CUT] for k in range(tokens // CUT)], axis=0)


def two_heads(even, odd):
    return jnp.where(iota(even.shape, 1) < HEAD, even, odd)


def end_state_kernel(
    x_hbm, b_hbm, c_hbm, step_hbm, keep_hbm,
    out_ref, x_ref, b_ref, c_ref, step_ref, keep_ref,
    x_rest, factor, lhs, sems,
):
    half = x_ref.shape[0]
    copies = [
        pltpu.make_async_copy(source, target, sems.at[i])
        for i, (source, target) in enumerate(
            (
                (keep_hbm, keep_ref),
                (step_hbm, step_ref),
                (b_hbm, b_ref),
                (x_hbm.at[pl.ds(0, half)], x_ref),
                (x_hbm.at[pl.ds(half, half)], x_rest),
                (c_hbm, c_ref),
            )
        )
    ]
    for copy in copies:
        copy.start()
    heads, tokens = step_ref.shape
    cuts = tokens // CUT
    row, col = iota((CUT, 2 * CUT), 0), iota((CUT, 2 * CUT), 1)
    kept = jnp.where((row > col) | (col >= CUT), 1.0, 0.0)
    copies[0].wait()
    sums = sum_of_pieces(by_cut(keep_ref), kept)
    after, total = sums[:, :CUT], sums[:, CUT:]
    count = heads * cuts
    row, col = iota((count, count), 0), iota((count, count), 1)
    same = row % heads == col % heads
    later = exact(jnp.where(same & (col // heads > row // heads), 1.0, 0.0), total)
    decay = jnp.exp(later[:heads] + total[:heads])
    lane = iota((1, CUT), 1) // (CUT // heads)
    decays = jnp.zeros((1, CUT), f32)
    for h in range(heads):
        decays = jnp.where(lane == h, decay[h : h + 1], decays)
    copies[1].wait()
    factor[...] = jnp.exp(after + later) * by_cut(step_ref)
    copies[2].wait()
    for k in range(cuts):
        part = b_ref[:, k * CUT : (k + 1) * CUT].astype(f32)
        for h in range(heads):
            scaled = part * factor[k * heads + h : k * heads + h + 1, :]
            lhs[h * STATE : (h + 1) * STATE, k * CUT : (k + 1) * CUT] = scaled.astype(bf16)
    copies[3].wait()
    copies[4].wait()
    pairs = heads // 2
    for pair in range(pairs):
        lanes = slice(pair * CUT, (pair + 1) * CUT)
        rows = slice(pair * 2 * STATE, (pair + 1) * 2 * STATE)
        both = dot(lhs[rows, :half], x_ref[:, lanes]) + dot(lhs[rows, half:], x_rest[:, lanes])
        out_ref[:, 0, lanes] = two_heads(both[:STATE], both[STATE:])
    out_ref[:, 0, pairs * CUT :] = jnp.broadcast_to(decays, (STATE, CUT))
    copies[5].wait()


def scan_kernel(heads, first, got_ref, _, out_ref, flag_ref, state_ref, decay_ref):
    flag_ref[...] = jnp.zeros_like(flag_ref)
    count = got_ref.shape[0]
    width = heads * HEAD
    state_ref[...] = got_ref[:, 0, :width]
    row, col = iota((CUT, width), 0), iota((CUT, width), 1)
    spread = jnp.where(row == col // HEAD * (CUT // heads), 1.0, 0.0)
    decay_ref[...] = exact(got_ref[:, 0, width:], spread)
    state = jnp.zeros((1, width), f32)
    for k in range(count):
        at = (k - first) % count
        out_ref[at] = state
        state = decay_ref[at : at + 1, :] * state + state_ref[at : at + 1, :]


def tile_copies(skipped, pairs, sems):
    def copies(k):
        source = pl.ds(pl.multiple_of((skipped + k) * CUT, CUT), CUT)
        at = pl.ds(pl.multiple_of(k * CUT, CUT), CUT)
        return [
            pltpu.make_async_copy(far.at[source], near.at[at], sems.at[i, k])
            for i, (far, near) in enumerate(pairs)
        ]

    def wait(k):
        for copy in copies(k):
            copy.wait()

    for k in range(pairs[0][1].shape[0] // CUT):
        for copy in copies(k):
            copy.start()
    return wait


def early_kernel(
    skip_ref, x_ref, b_ref, c_ref, step_ref, keep_ref, gate_hbm,
    base_ref, carry_ref, state_out, gate_ref, *rest,
):
    *scratch, state, sems = rest
    wait = tile_copies(0, [(gate_hbm, gate_ref)], sems)
    state[...] = jnp.zeros_like(state)
    cut_by_cut(
        0, skip_ref, x_ref, gate_ref, b_ref, c_ref, step_ref, keep_ref, base_ref, carry_ref,
        *scratch, state, wait, lambda: None,
    )
    state_out[...] = state[...]


def late_kernel(
    flag_ref, state_in, skip_ref, x_hbm, b_hbm, c_hbm, step_hbm, keep_hbm, gate_hbm,
    base_ref, carry_ref, gate_ref, *rest,
):
    *scratch, state, sems, x_ref, b_ref, c_ref, step_ref, keep_ref, more_sems = rest
    copies = [
        pltpu.make_async_copy(far, near, more_sems.at[i])
        for i, (far, near) in enumerate(
            ((keep_hbm, keep_ref), (step_hbm, step_ref), (b_hbm, b_ref), (c_hbm, c_ref))
        )
    ]
    for copy in copies:
        copy.start()
    skipped = x_ref.shape[0] // CUT
    wait = tile_copies(skipped, [(x_hbm, x_ref), (gate_hbm, gate_ref)], sems)
    state[...] = state_in[...]
    copies[0].wait()
    copies[1].wait()

    def wait_both():
        copies[2].wait()
        copies[3].wait()

    cut_by_cut(
        skipped, skip_ref, x_ref, gate_ref, b_ref, c_ref, step_ref, keep_ref,
        base_ref, carry_ref, *scratch, state, wait, wait_both,
    )


def cut_by_cut(
    skipped, skip_ref, x_ref, gate_ref, b_ref, c_ref, step_ref, keep_ref, base_ref, carry_ref,
    left, offset, factor, decays, starts, state, wait_tile, wait_rest,
):
    heads, tokens = step_ref.shape
    cuts = tokens // CUT
    mine = x_ref.shape[0] // CUT
    count = heads * cuts
    step = by_cut(step_ref)
    row, col = iota((CUT, 3 * CUT), 0), iota((CUT, 3 * CUT), 1)
    kind = col // CUT
    kept = (kind == 2) | ((kind == 0) & (row <= col)) | ((kind == 1) & (row > col - CUT))
    sums = sum_of_pieces(by_cut(keep_ref), jnp.where(kept, 1.0, 0.0))
    upto, after, total = (sums[:, i * CUT : (i + 1) * CUT] for i in range(3))
    upto = upto * LOG2E
    row, col = iota((count, count), 0), iota((count, count), 1)
    earlier_cut = (row % heads == col % heads) & (col // heads < row // heads)
    factor[...] = jnp.exp(after) * step
    decays[...] = jnp.exp(total)
    starts[...] = jnp.exp(exact(jnp.where(earlier_cut, 1.0, 0.0), total))
    offset[...] = jnp.log2(jnp.maximum(step, 1e-37)) - upto
    for k in range(mine):
        rows = upto[(skipped + k) * heads : (skipped + k + 1) * heads]
        left[k] = jnp.concatenate([rows, jnp.zeros((8 - heads, CUT), f32)], axis=0)
    row, col = iota((CUT, CUT), 0), iota((CUT, CUT), 1)
    causal = row >= col
    low_lanes = jnp.where(iota((1, CUT), 1) < HEAD, 1.0, 0.0)
    only = [low_lanes.astype(bf16), (1.0 - low_lanes).astype(bf16)]

    def one_cut(k, _):
        at = pl.ds(pl.multiple_of(k * CUT, CUT), CUT)
        far = pl.ds(pl.multiple_of((skipped + k) * CUT, CUT), CUT)
        first = (skipped + k) * heads
        wait_tile(k)
        b = b_ref[:, far]
        c = jnp.transpose(c_ref[:, far])
        growths = jnp.transpose(left[k])
        growths = [jnp.broadcast_to(growths[:, h : h + 1], (CUT, CUT)) for h in range(heads)]
        scores = jnp.where(causal, dot(c, b), 0.0)
        b_turned = b.astype(f32)
        now = state[...]
        high = now.astype(bf16)
        low = (now - high.astype(f32)).astype(bf16)
        earlier = dot(jnp.concatenate([c, c], axis=1), jnp.concatenate([high, low], axis=0))
        for pair in range(heads // 2):
            lanes = slice(pair * CUT, (pair + 1) * CUT)
            x = x_ref[at, lanes]
            weights = []
            for h in range(2 * pair, 2 * pair + 2):
                gaps = growths[h] + offset[pl.ds(first + h, 1), :]
                weights.append((scores * jnp.exp2(jnp.minimum(gaps, 0.0))).astype(bf16))
            inside = dot(
                jnp.concatenate(weights, axis=1), jnp.concatenate([x * mask for mask in only], axis=0)
            )
            growth = jnp.exp2(two_heads(growths[2 * pair], growths[2 * pair + 1]))
            gate = gate_ref[at, lanes].astype(f32)
            gate = gate * pl.reciprocal(1.0 + jnp.exp(-gate))
            skip = two_heads(
                jnp.full((1, CUT), skip_ref[2 * pair]), jnp.full((1, CUT), skip_ref[2 * pair + 1])
            )
            base_ref[at, lanes] = (inside + growth * earlier[:, lanes] + skip * x.astype(f32)) * gate

            def per_channel(ref):
                even = first + 2 * pair
                return two_heads(ref[pl.ds(even, 1), :], ref[pl.ds(even + 1, 1), :])

            carry_ref[at, lanes] = (growth * per_channel(starts) * gate).astype(bf16)
            scaled = [b_turned * factor[pl.ds(first + 2 * pair + i, 1), :] for i in range(2)]
            both = dot(jnp.concatenate(scaled, axis=0).astype(bf16), x)
            state[:, lanes] = per_channel(decays) * now[:, lanes] + two_heads(both[:STATE], both[STATE:])
        return 0

    wait_rest()
    lax.fori_loop(0, mine, one_cut, 0, unroll=UNROLL)


def gate_kernel(got_ref, c_ref, *refs):
    *parts, gated_ref, squares_ref = refs
    peers = squares_ref.shape[0]
    tokens = gated_ref.shape[0]
    now = got_ref[:, 0, :]
    high = now.astype(bf16)
    low = (now - high.astype(f32)).astype(bf16)
    both = jnp.concatenate([high, low], axis=0)
    ones = jnp.ones((8, 2 * CUT), bf16)
    size = 2 * CUT
    half_tokens = tokens // (len(parts) // 2)
    for k in range(tokens // size):
        at = slice(k * size, (k + 1) * size)
        c = c_ref[:, at]
        added = dot_tn(jnp.concatenate([c, c], axis=0), both)
        first = k * size
        base_ref, carry_ref = parts[2 * (first // half_tokens) : 2 * (first // half_tokens) + 2]
        here = slice(first % half_tokens, first % half_tokens + size)
        gated = base_ref[here, :] + carry_ref[here, :].astype(f32) * added
        gated_ref[at, :] = gated
        square = gated * gated
        square = square[:, :CUT] + square[:, CUT:]
        high = square.astype(bf16)
        low = (square - high.astype(f32)).astype(bf16)
        summed = dot_nt(ones, jnp.concatenate([high, low], axis=1))
        for peer in range(peers):
            for half in range(2):
                squares_ref[peer, 2 * k + half : 2 * k + half + 1, :] = summed[
                    :1, half * CUT : (half + 1) * CUT
                ]


def norm_kernel(got_ref, gain_ref, gated_ref, out_hbm, out_ref, sems):
    peers = got_ref.shape[0]
    cuts = got_ref.shape[1]
    summed = got_ref[0]
    for peer in range(1, peers):
        summed = summed + got_ref[peer]
    pieces = split3(lax.rsqrt(summed / CH + EPSILON))
    gain = gain_ref[...]
    ones = jnp.where(iota((8, gain.shape[1]), 0) < 3, 1.0, 0.0).astype(bf16)
    copies = []
    for k in range(cuts):
        at = slice(k * CUT, (k + 1) * CUT)
        rows = [piece[k : k + 1] for piece in pieces] + [jnp.zeros((5, CUT), f32)]
        factor = dot(jnp.transpose(jnp.concatenate(rows, axis=0)).astype(bf16), ones)
        out_ref[at, :] = (gated_ref[at, :] * factor * gain).astype(bf16)
        if k % 4 == 3:
            four = pl.ds((k - 3) * CUT, 4 * CUT)
            copy = pltpu.make_async_copy(out_ref.at[four], out_hbm.at[four], sems.at[k // 4])
            copy.start()
            copies.append(copy)
    for copy in copies:
        copy.wait()


VMEM = pl.BlockSpec(memory_space=pltpu.VMEM)
SMEM = pl.BlockSpec(memory_space=pltpu.SMEM)
HBM = pl.BlockSpec(memory_space=pltpu.HBM)


def call(kernel, out_shape, in_specs, scratch=(), out_specs=None, flops=1000000):
    return pl.pallas_call(
        kernel,
        out_shape=out_shape,
        in_specs=in_specs,
        out_specs=out_specs or jax.tree.map(lambda _: VMEM, out_shape),
        scratch_shapes=list(scratch),
        cost_estimate=pl.CostEstimate(flops=flops, bytes_accessed=4 * MIB, transcendentals=0),
        compiler_params=pltpu.CompilerParams(vmem_limit_bytes=16 * MIB),
    )


def exchange(v, axis):
    size, first = lax.axis_size(axis), FIRST[axis]
    places = [[(first + k) % size for k in range(size)]]
    return lax.all_to_all(v, axis, 0, 0, axis_index_groups=places, tiled=True)


def per_device(x_in, gate_in, b_in, c_in, step_size, log_keep, skip_gain, norm_gain):
    tokens, channels = x_in.shape
    heads = step_size.shape[0]
    cuts = tokens // CUT
    shape = jax.ShapeDtypeStruct
    dma = pltpu.SemaphoreType.DMA
    b_turned, c_turned = b_in.T, c_in.T
    x_in, gate_in, b_turned, c_far, step_size, log_keep, skip_gain = (
        pltpu.with_memory_space_constraint(v, pltpu.HBM)
        for v in (x_in, gate_in, b_turned, c_turned, step_size, log_keep, skip_gain)
    )
    rows = pltpu.VMEM((heads * cuts, CUT), f32)
    half = tokens // 2
    row = pltpu.VMEM((STATE, channels), f32)
    part = shape((half, channels), bf16)
    turned = shape((STATE, tokens), bf16)
    per_head = shape((heads, tokens), f32)
    near_shapes = (turned, turned, per_head, per_head)
    local_shapes = (shape((half, channels), f32), part)
    half_wide = pltpu.VMEM((half, channels), bf16)
    local_scratch = [
        half_wide,
        pltpu.VMEM((cuts // 2, 8, CUT), f32),
        rows,
        rows, rows, rows, row,
    ]
    message, x_near, *near = call(
        end_state_kernel,
        (shape((STATE, 1, channels + CUT), f32), part, *near_shapes),
        [HBM] * 5,
        [half_wide, rows, pltpu.VMEM((heads * STATE, tokens), bf16), dma((6,))],
        flops=2 * tokens * STATE * channels,
    )(x_in, b_turned, c_far, step_size, log_keep)
    got = exchange(message, SEQ)
    base_0, carry_0, state = call(
        early_kernel,
        (*local_shapes, shape((STATE, channels), f32)),
        [SMEM] + [VMEM] * 5 + [HBM],
        [*local_scratch, dma((1, cuts // 2))],
        flops=int(5e9),
    )(skip_gain, x_near, *near, gate_in)
    before, flag = call(
        functools.partial(scan_kernel, heads, FIRST["seq"]),
        (shape((STATE, 1, channels), f32), shape((8, CUT), f32)),
        [VMEM] * 2,
        [row, row],
    )(got, state)
    entering = exchange(before, SEQ)
    base_1, carry_1 = call(
        late_kernel,
        local_shapes,
        [VMEM] * 2 + [SMEM] + [HBM] * 6,
        [
            *local_scratch, dma((2, cuts // 2)), half_wide,
            *(pltpu.VMEM(v.shape, v.dtype) for v in near_shapes), dma((4,)),
        ],
        flops=int(5e9),
    )(flag, state, skip_gain, x_in, b_turned, c_far, step_size, log_keep, gate_in)
    peers = lax.axis_size("chan")
    gated, squares = call(
        gate_kernel,
        (shape((tokens, channels), f32), shape((peers, cuts, CUT), f32)),
        [VMEM] * 6,
        flops=2 * tokens * STATE * channels,
    )(entering, c_turned, base_0, carry_0, base_1, carry_1)
    summed = exchange(squares, "chan")
    return call(
        norm_kernel,
        shape((tokens, channels), bf16),
        [VMEM] * 3,
        [pltpu.VMEM((tokens, channels), bf16), dma((4,))],
        out_specs=HBM,
    )(summed, norm_gain.reshape(1, channels), gated)


def solution(mesh):
    placed = (
        P(SEQ, "chan"),
        P(SEQ, "chan"),
        P(SEQ, None),
        P(SEQ, None),
        P("chan", SEQ),
        P("chan", SEQ),
        P("chan"),
        P("chan"),
    )
    return jax.shard_map(
        per_device, mesh=mesh, in_specs=placed, out_specs=P(SEQ, "chan"), check_vma=False
    )
```

```python
import functools

import jax
import jax.numpy as jnp
from jax import lax
from jax.experimental import pallas as pl
from jax.experimental.pallas import tpu as pltpu
from jax.sharding import PartitionSpec as P

CH = 2048
HEAD = 64
STATE = 64
SEQ = "seq"
CUT = 128
EPSILON = 1e-05
LOG2E = 1.4426950408889634
MIB = 1024 * 1024
UNROLL = 4
FIRST = {"seq": 45, "chan": 5}

f32 = jnp.float32
bf16 = jnp.bfloat16
exact = functools.partial(
    jnp.dot, precision=lax.Precision.HIGHEST, preferred_element_type=f32
)


def dot(a, b):
    return jnp.dot(a, b, preferred_element_type=f32)


def dot_nt(a, b):
    return lax.dot_general(a, b, (((1,), (1,)), ((), ())), preferred_element_type=f32)


def dot_tn(a, b):
    return lax.dot_general(a, b, (((0,), (0,)), ((), ())), preferred_element_type=f32)


def iota(shape, axis):
    return lax.broadcasted_iota(jnp.int32, shape, axis)


def split3(v):
    high = v.astype(bf16).astype(f32)
    rest = v - high
    middle = rest.astype(bf16).astype(f32)
    return high, middle, rest - middle


def sum_of_pieces(v, zeros_and_ones):
    ones = zeros_and_ones.astype(bf16)
    high, middle, low = (dot(piece.astype(bf16), ones) for piece in split3(v))
    return high + (middle + low)


def by_cut(ref):
    tokens = ref.shape[1]
    return jnp.concatenate([ref[:, k * CUT : (k + 1) * CUT] for k in range(tokens // CUT)], axis=0)


def two_heads(even, odd):
    return jnp.where(iota(even.shape, 1) < HEAD, even, odd)


def end_state_kernel(
    x_hbm, b_hbm, c_hbm, step_hbm, keep_hbm,
    out_ref, x_ref, b_ref, c_ref, step_ref, keep_ref,
    x_rest, factor, sems,
):
    half = x_ref.shape[0]
    copies = [
        pltpu.make_async_copy(source, target, sems.at[i])
        for i, (source, target) in enumerate(
            (
                (keep_hbm, keep_ref),
                (step_hbm, step_ref),
                (b_hbm, b_ref),
                (x_hbm.at[pl.ds(0, half)], x_ref),
                (x_hbm.at[pl.ds(half, half)], x_rest),
                (c_hbm, c_ref),
            )
        )
    ]
    for copy in copies:
        copy.start()
    heads, tokens = step_ref.shape
    cuts = tokens // CUT
    row, col = iota((CUT, 2 * CUT), 0), iota((CUT, 2 * CUT), 1)
    kept = jnp.where((row > col) | (col >= CUT), 1.0, 0.0)
    copies[0].wait()
    sums = sum_of_pieces(by_cut(keep_ref), kept)
    after, total = sums[:, :CUT], sums[:, CUT:]
    count = heads * cuts
    row, col = iota((count, count), 0), iota((count, count), 1)
    same = row % heads == col % heads
    mask = jnp.where(same & (col // heads > row // heads), 1.0, 0.0).astype(bf16)
    later = sum(dot(mask, piece.astype(bf16)) for piece in reversed(split3(total)))
    decay = jnp.exp(later[:heads] + total[:heads])
    lane = iota((1, CUT), 1) // (CUT // heads)
    decays = jnp.zeros((1, CUT), f32)
    for h in range(heads):
        decays = jnp.where(lane == h, decay[h : h + 1], decays)
    copies[1].wait()
    factor[...] = jnp.exp(after + later) * by_cut(step_ref)
    copies[2].wait()
    pairs = heads // 2
    both = [jnp.zeros((2 * STATE, CUT), f32)] * pairs
    for k in range(0, cuts, 2):
        at = k * CUT
        near = x_ref if at < half else x_rest
        if at % half == 0:
            copies[3 + at // half].wait()
        part = b_ref[:, at : at + 2 * CUT].astype(f32)
        for pair in range(pairs):
            lhs = []
            for h in range(2 * pair, 2 * pair + 2):
                rows = [factor[(k + i) * heads + h : (k + i) * heads + h + 1, :] for i in range(2)]
                lhs.append((part * jnp.concatenate(rows, axis=1)).astype(bf16))
            x = near[at % half : at % half + 2 * CUT, pair * CUT : (pair + 1) * CUT]
            both[pair] = both[pair] + dot(jnp.concatenate(lhs, axis=0), x)
    for pair in range(pairs):
        lanes = slice(pair * CUT, (pair + 1) * CUT)
        out_ref[:, 0, lanes] = two_heads(both[pair][:STATE], both[pair][STATE:])
    out_ref[:, 0, pairs * CUT :] = jnp.broadcast_to(decays, (STATE, CUT))
    copies[5].wait()


def scan_kernel(heads, first, got_ref, _, out_ref, flag_ref, *refs):
    flag_ref[...] = jnp.zeros_like(flag_ref)
    count = got_ref.shape[0]
    width = heads * HEAD
    seam = count - first

    def rolled(lanes):
        return jnp.concatenate([got_ref[seam:, 0, lanes], got_ref[:seam, 0, lanes]], axis=0)

    row, col = iota((CUT, width), 0), iota((CUT, width), 1)
    spread = jnp.where(row == col // HEAD * (CUT // heads), 1.0, 0.0)
    all_decays = sum_of_pieces(rolled(slice(width, width + CUT)), spread)
    groups = 8
    steps = count // groups
    for part in range(width // CUT):
        lanes = slice(part * CUT, (part + 1) * CUT)
        state_ref, decay_ref = refs[2 * part : 2 * part + 2]
        state_ref[...] = rolled(lanes)
        decay_ref[...] = all_decays[:, lanes]
        states, decays = [], []
        for j in range(steps):
            at = pl.ds(j, groups, stride=steps)
            state, decay = state_ref[at, :], decay_ref[at, :]
            if j:
                state, decay = state + decay * states[-1], decay * decays[-1]
            states.append(state)
            decays.append(decay)
        carries = [jnp.zeros((1, CUT), f32)]
        for g in range(groups - 1):
            carries.append(decays[-1][g : g + 1] * carries[-1] + states[-1][g : g + 1])
        carry = jnp.concatenate(carries, axis=0)
        for j in range(steps):
            before = states[j - 1] + decays[j - 1] * carry if j else carry
            state_ref[pl.ds(j, groups, stride=steps), :] = before
        out_ref[seam:, 0, lanes] = state_ref[:first, :]
        out_ref[:seam, 0, lanes] = state_ref[first:, :]


def tile_copies(skipped, pairs, sems):
    def copies(k):
        source = pl.ds(pl.multiple_of((skipped + k) * CUT, CUT), CUT)
        at = pl.ds(pl.multiple_of(k * CUT, CUT), CUT)
        return [
            pltpu.make_async_copy(far.at[source], near.at[at], sems.at[i, k])
            for i, (far, near) in enumerate(pairs)
        ]

    def wait(k):
        for copy in copies(k):
            copy.wait()

    for k in range(pairs[0][1].shape[0] // CUT):
        for copy in copies(k):
            copy.start()
    return wait


def early_kernel(
    skip_ref, x_ref, b_ref, c_ref, step_ref, keep_ref, gate_hbm,
    base_ref, carry_ref, state_out, gate_ref, *rest,
):
    *scratch, state, sems = rest
    wait = tile_copies(0, [(gate_hbm, gate_ref)], sems)
    state[...] = jnp.zeros_like(state)
    cut_by_cut(
        0, skip_ref, x_ref, gate_ref, b_ref, c_ref, step_ref, keep_ref, base_ref, carry_ref,
        *scratch, state, wait, lambda: None,
    )
    state_out[...] = state[...]


def late_kernel(
    flag_ref, state_in, skip_ref, x_hbm, b_hbm, c_hbm, step_hbm, keep_hbm, gate_hbm,
    base_ref, carry_ref, gate_ref, *rest,
):
    *scratch, state, sems, x_ref, b_ref, c_ref, step_ref, keep_ref, more_sems = rest
    copies = [
        pltpu.make_async_copy(far, near, more_sems.at[i])
        for i, (far, near) in enumerate(
            ((keep_hbm, keep_ref), (step_hbm, step_ref), (b_hbm, b_ref), (c_hbm, c_ref))
        )
    ]
    for copy in copies:
        copy.start()
    skipped = x_ref.shape[0] // CUT
    wait = tile_copies(skipped, [(x_hbm, x_ref), (gate_hbm, gate_ref)], sems)
    state[...] = state_in[...]
    copies[0].wait()
    copies[1].wait()

    def wait_both():
        copies[2].wait()
        copies[3].wait()

    cut_by_cut(
        skipped, skip_ref, x_ref, gate_ref, b_ref, c_ref, step_ref, keep_ref,
        base_ref, carry_ref, *scratch, state, wait, wait_both,
    )


def cut_by_cut(
    skipped, skip_ref, x_ref, gate_ref, b_ref, c_ref, step_ref, keep_ref, base_ref, carry_ref,
    left, offset, factor, decays, starts, state, wait_tile, wait_rest,
):
    heads, tokens = step_ref.shape
    cuts = tokens // CUT
    mine = x_ref.shape[0] // CUT
    count = heads * cuts
    step = by_cut(step_ref)
    row, col = iota((CUT, 3 * CUT), 0), iota((CUT, 3 * CUT), 1)
    kind = col // CUT
    kept = (kind == 2) | ((kind == 0) & (row <= col)) | ((kind == 1) & (row > col - CUT))
    sums = sum_of_pieces(by_cut(keep_ref), jnp.where(kept, 1.0, 0.0))
    upto, after, total = (sums[:, i * CUT : (i + 1) * CUT] for i in range(3))
    upto = upto * LOG2E
    row, col = iota((count, count), 0), iota((count, count), 1)
    earlier_cut = (row % heads == col % heads) & (col // heads < row // heads)
    factor[...] = jnp.exp(after) * step
    decays[...] = jnp.exp(total)
    starts[...] = jnp.exp(exact(jnp.where(earlier_cut, 1.0, 0.0), total))
    offset[...] = jnp.log2(jnp.maximum(step, 1e-37)) - upto
    for k in range(mine):
        rows = upto[(skipped + k) * heads : (skipped + k + 1) * heads]
        left[k] = jnp.concatenate([rows, jnp.zeros((8 - heads, CUT), f32)], axis=0)
    row, col = iota((CUT, CUT), 0), iota((CUT, CUT), 1)
    causal = row >= col
    low_lanes = jnp.where(iota((1, CUT), 1) < HEAD, 1.0, 0.0)
    only = [low_lanes.astype(bf16), (1.0 - low_lanes).astype(bf16)]

    def one_cut(k, _):
        at = pl.ds(pl.multiple_of(k * CUT, CUT), CUT)
        far = pl.ds(pl.multiple_of((skipped + k) * CUT, CUT), CUT)
        first = (skipped + k) * heads
        b = b_ref[:, far]
        c = jnp.transpose(c_ref[:, far])
        growths = jnp.transpose(left[k])
        growths = [jnp.broadcast_to(growths[:, h : h + 1], (CUT, CUT)) for h in range(heads)]
        scores = jnp.where(causal, dot(c, b), 0.0)
        b_turned = b.astype(f32)
        now = state[...]
        high = now.astype(bf16)
        low = (now - high.astype(f32)).astype(bf16)
        earlier = dot(jnp.concatenate([c, c], axis=1), jnp.concatenate([high, low], axis=0))
        for pair in range(heads // 2):
            lanes = slice(pair * CUT, (pair + 1) * CUT)
            x = x_ref[at, lanes]
            weights = []
            for h in range(2 * pair, 2 * pair + 2):
                gaps = growths[h] + offset[pl.ds(first + h, 1), :]
                weights.append((scores * jnp.exp2(jnp.minimum(gaps, 0.0))).astype(bf16))
            inside = dot(
                jnp.concatenate(weights, axis=1), jnp.concatenate([x * mask for mask in only], axis=0)
            )
            growth = jnp.exp2(two_heads(growths[2 * pair], growths[2 * pair + 1]))
            gate = gate_ref[at, lanes].astype(f32)
            gate = gate * pl.reciprocal(1.0 + jnp.exp(-gate))
            skip = two_heads(
                jnp.full((1, CUT), skip_ref[2 * pair]), jnp.full((1, CUT), skip_ref[2 * pair + 1])
            )
            base_ref[at, lanes] = (inside + growth * earlier[:, lanes] + skip * x.astype(f32)) * gate

            def per_channel(ref):
                even = first + 2 * pair
                return two_heads(ref[pl.ds(even, 1), :], ref[pl.ds(even + 1, 1), :])

            carry_ref[at, lanes] = (growth * per_channel(starts) * gate).astype(bf16)
            scaled = [b_turned * factor[pl.ds(first + 2 * pair + i, 1), :] for i in range(2)]
            both = dot(jnp.concatenate(scaled, axis=0).astype(bf16), x)
            state[:, lanes] = per_channel(decays) * now[:, lanes] + two_heads(both[:STATE], both[STATE:])
        return 0

    wait_rest()
    for k in range(mine):
        wait_tile(k)
    lax.fori_loop(0, mine, one_cut, 0, unroll=UNROLL)


def gate_kernel(got_ref, c_ref, *refs):
    *parts, gated_ref, squares_ref = refs
    peers = squares_ref.shape[0]
    tokens = gated_ref.shape[0]
    now = got_ref[:, 0, :]
    high = now.astype(bf16)
    low = (now - high.astype(f32)).astype(bf16)
    both = jnp.concatenate([high, low], axis=0)
    ones = jnp.ones((8, 2 * CUT), bf16)
    size = 2 * CUT
    half_tokens = tokens // (len(parts) // 2)
    for k in range(tokens // size):
        at = slice(k * size, (k + 1) * size)
        c = c_ref[:, at]
        added = dot_tn(jnp.concatenate([c, c], axis=0), both)
        first = k * size
        base_ref, carry_ref = parts[2 * (first // half_tokens) : 2 * (first // half_tokens) + 2]
        here = slice(first % half_tokens, first % half_tokens + size)
        gated = base_ref[here, :] + carry_ref[here, :].astype(f32) * added
        gated_ref[at, :] = gated
        square = gated * gated
        square = square[:, :CUT] + square[:, CUT:]
        high = square.astype(bf16)
        low = (square - high.astype(f32)).astype(bf16)
        summed = dot_nt(ones, jnp.concatenate([high, low], axis=1))
        for peer in range(peers):
            for half in range(2):
                squares_ref[peer, 2 * k + half : 2 * k + half + 1, :] = summed[
                    :1, half * CUT : (half + 1) * CUT
                ]


def norm_kernel(got_ref, gain_ref, gated_ref, out_hbm, out_ref, sems):
    peers = got_ref.shape[0]
    cuts = got_ref.shape[1]
    summed = got_ref[0]
    for peer in range(1, peers):
        summed = summed + got_ref[peer]
    pieces = split3(lax.rsqrt(summed / CH + EPSILON))
    gain = gain_ref[...]
    ones = jnp.where(iota((8, gain.shape[1]), 0) < 3, 1.0, 0.0).astype(bf16)
    copies = []
    for k in range(cuts):
        at = slice(k * CUT, (k + 1) * CUT)
        rows = [piece[k : k + 1] for piece in pieces] + [jnp.zeros((5, CUT), f32)]
        factor = dot(jnp.transpose(jnp.concatenate(rows, axis=0)).astype(bf16), ones)
        out_ref[at, :] = (gated_ref[at, :] * factor * gain).astype(bf16)
        if k % 2 == 1:
            two = pl.ds((k - 1) * CUT, 2 * CUT)
            copy = pltpu.make_async_copy(out_ref.at[two], out_hbm.at[two], sems.at[k // 2])
            copy.start()
            copies.append(copy)
    for copy in copies:
        copy.wait()


VMEM = pl.BlockSpec(memory_space=pltpu.VMEM)
SMEM = pl.BlockSpec(memory_space=pltpu.SMEM)
HBM = pl.BlockSpec(memory_space=pltpu.HBM)


def call(kernel, out_shape, in_specs, scratch=(), out_specs=None, flops=1000000):
    return pl.pallas_call(
        kernel,
        out_shape=out_shape,
        in_specs=in_specs,
        out_specs=out_specs or jax.tree.map(lambda _: VMEM, out_shape),
        scratch_shapes=list(scratch),
        cost_estimate=pl.CostEstimate(flops=flops, bytes_accessed=4 * MIB, transcendentals=0),
        compiler_params=pltpu.CompilerParams(vmem_limit_bytes=16 * MIB),
    )


def exchange(v, axis):
    size, first = lax.axis_size(axis), FIRST[axis]
    places = [[(first + k) % size for k in range(size)]]
    return lax.all_to_all(v, axis, 0, 0, axis_index_groups=places, tiled=True)


def per_device(x_in, gate_in, b_in, c_in, step_size, log_keep, skip_gain, norm_gain):
    tokens, channels = x_in.shape
    heads = step_size.shape[0]
    cuts = tokens // CUT
    shape = jax.ShapeDtypeStruct
    dma = pltpu.SemaphoreType.DMA
    b_turned, c_turned = b_in.T, c_in.T
    x_in, gate_in, b_turned, c_far, step_size, log_keep, skip_gain = (
        pltpu.with_memory_space_constraint(v, pltpu.HBM)
        for v in (x_in, gate_in, b_turned, c_turned, step_size, log_keep, skip_gain)
    )
    rows = pltpu.VMEM((heads * cuts, CUT), f32)
    half = tokens // 2
    row = pltpu.VMEM((STATE, channels), f32)
    part = shape((half, channels), bf16)
    turned = shape((STATE, tokens), bf16)
    per_head = shape((heads, tokens), f32)
    near_shapes = (turned, turned, per_head, per_head)
    local_shapes = (shape((half, channels), f32), part)
    half_wide = pltpu.VMEM((half, channels), bf16)
    local_scratch = [
        half_wide,
        pltpu.VMEM((cuts // 2, 8, CUT), f32),
        rows,
        rows, rows, rows, row,
    ]
    message, x_near, *near = call(
        end_state_kernel,
        (shape((STATE, 1, channels + CUT), f32), part, *near_shapes),
        [HBM] * 5,
        [half_wide, rows, dma((6,))],
        flops=2 * tokens * STATE * channels,
    )(x_in, b_turned, c_far, step_size, log_keep)
    got = exchange(message, SEQ)
    base_0, carry_0, state = call(
        early_kernel,
        (*local_shapes, shape((STATE, channels), f32)),
        [SMEM] + [VMEM] * 5 + [HBM],
        [*local_scratch, dma((1, cuts // 2))],
        flops=int(5e9),
    )(skip_gain, x_near, *near, gate_in)
    before, flag = call(
        functools.partial(scan_kernel, heads, FIRST["seq"]),
        (shape((STATE, 1, channels), f32), shape((8, CUT), f32)),
        [VMEM] * 2,
        [pltpu.VMEM((STATE, CUT), f32)] * (2 * channels // CUT),
    )(got, state)
    entering = exchange(before, SEQ)
    base_1, carry_1 = call(
        late_kernel,
        local_shapes,
        [VMEM] * 2 + [SMEM] + [HBM] * 6,
        [
            *local_scratch, dma((2, cuts // 2)), half_wide,
            *(pltpu.VMEM(v.shape, v.dtype) for v in near_shapes), dma((4,)),
        ],
        flops=int(5e9),
    )(flag, state, skip_gain, x_in, b_turned, c_far, step_size, log_keep, gate_in)
    peers = lax.axis_size("chan")
    gated, squares = call(
        gate_kernel,
        (shape((tokens, channels), f32), shape((peers, cuts, CUT), f32)),
        [VMEM] * 6,
        flops=2 * tokens * STATE * channels,
    )(entering, c_turned, base_0, carry_0, base_1, carry_1)
    summed = exchange(squares, "chan")
    return call(
        norm_kernel,
        shape((tokens, channels), bf16),
        [VMEM] * 3,
        [pltpu.VMEM((tokens, channels), bf16), dma((cuts // 2,))],
        out_specs=HBM,
    )(summed, norm_gain.reshape(1, channels), gated)


def solution(mesh):
    placed = (
        P(SEQ, "chan"),
        P(SEQ, "chan"),
        P(SEQ, None),
        P(SEQ, None),
        P("chan", SEQ),
        P("chan", SEQ),
        P("chan"),
        P("chan"),
    )
    return jax.shard_map(
        per_device, mesh=mesh, in_specs=placed, out_specs=P(SEQ, "chan"), check_vma=False
    )
```

```python
import functools

import jax
import jax.numpy as jnp
from jax import lax
from jax.experimental import pallas as pl
from jax.experimental.pallas import tpu as pltpu
from jax.sharding import PartitionSpec as P

CH = 2048
HEAD = 64
STATE = 64
SEQ = "seq"
CUT = 128
EPSILON = 1e-05
LOG2E = 1.4426950408889634
MIB = 1024 * 1024
UNROLL = 4
FIRST = {"seq": 47, "chan": 5}

f32 = jnp.float32
bf16 = jnp.bfloat16
exact = functools.partial(
    jnp.dot, precision=lax.Precision.HIGHEST, preferred_element_type=f32
)


def dot(a, b):
    return jnp.dot(a, b, preferred_element_type=f32)


def dot_nt(a, b):
    return lax.dot_general(a, b, (((1,), (1,)), ((), ())), preferred_element_type=f32)


def dot_tn(a, b):
    return lax.dot_general(a, b, (((0,), (0,)), ((), ())), preferred_element_type=f32)


def iota(shape, axis):
    return lax.broadcasted_iota(jnp.int32, shape, axis)


def split3(v):
    high = v.astype(bf16).astype(f32)
    rest = v - high
    middle = rest.astype(bf16).astype(f32)
    return high, middle, rest - middle


def sum_of_pieces(v, zeros_and_ones):
    ones = zeros_and_ones.astype(bf16)
    high, middle, low = (dot(piece.astype(bf16), ones) for piece in split3(v))
    return high + (middle + low)


def by_cut(ref):
    tokens = ref.shape[1]
    return jnp.concatenate([ref[:, k * CUT : (k + 1) * CUT] for k in range(tokens // CUT)], axis=0)


def two_heads(even, odd):
    return jnp.where(iota(even.shape, 1) < HEAD, even, odd)


def end_state_kernel(
    x_hbm, gate_hbm, b_hbm, c_hbm, step_hbm, keep_hbm,
    out_ref, x_ref, gate_ref, b_ref, c_ref, step_ref, keep_ref,
    x_rest, factor, sems,
):
    half = x_ref.shape[0]
    copies = [
        pltpu.make_async_copy(source, target, sems.at[i])
        for i, (source, target) in enumerate(
            (
                (keep_hbm, keep_ref),
                (step_hbm, step_ref),
                (b_hbm, b_ref),
                (x_hbm.at[pl.ds(0, half)], x_ref),
                (x_hbm.at[pl.ds(half, half)], x_rest),
                (c_hbm, c_ref),
                (gate_hbm.at[pl.ds(0, half)], gate_ref),
            )
        )
    ]
    for copy in copies:
        copy.start()
    heads, tokens = step_ref.shape
    cuts = tokens // CUT
    row, col = iota((CUT, 2 * CUT), 0), iota((CUT, 2 * CUT), 1)
    kept = jnp.where((row > col) | (col >= CUT), 1.0, 0.0)
    copies[0].wait()
    sums = sum_of_pieces(by_cut(keep_ref), kept)
    after, total = sums[:, :CUT], sums[:, CUT:]
    count = heads * cuts
    row, col = iota((count, count), 0), iota((count, count), 1)
    same = row % heads == col % heads
    mask = jnp.where(same & (col // heads > row // heads), 1.0, 0.0).astype(bf16)
    later = sum(dot(mask, piece.astype(bf16)) for piece in reversed(split3(total)))
    decay = jnp.exp(later[:heads] + total[:heads])
    lane = iota((1, CUT), 1) // (CUT // heads)
    decays = jnp.zeros((1, CUT), f32)
    for h in range(heads):
        decays = jnp.where(lane == h, decay[h : h + 1], decays)
    copies[1].wait()
    factor[...] = jnp.exp(after + later) * by_cut(step_ref)
    copies[2].wait()
    pairs = heads // 2
    both = [jnp.zeros((2 * STATE, CUT), f32)] * pairs
    for k in range(0, cuts, 2):
        at = k * CUT
        near = x_ref if at < half else x_rest
        if at % half == 0:
            copies[3 + at // half].wait()
        part = b_ref[:, at : at + 2 * CUT].astype(f32)
        for pair in range(pairs):
            lhs = []
            for h in range(2 * pair, 2 * pair + 2):
                rows = [factor[(k + i) * heads + h : (k + i) * heads + h + 1, :] for i in range(2)]
                lhs.append((part * jnp.concatenate(rows, axis=1)).astype(bf16))
            x = near[at % half : at % half + 2 * CUT, pair * CUT : (pair + 1) * CUT]
            both[pair] = both[pair] + dot(jnp.concatenate(lhs, axis=0), x)
    for pair in range(pairs):
        lanes = slice(pair * CUT, (pair + 1) * CUT)
        out_ref[:, 0, lanes] = two_heads(both[pair][:STATE], both[pair][STATE:])
    out_ref[:, 0, pairs * CUT :] = jnp.broadcast_to(decays, (STATE, CUT))
    copies[5].wait()
    copies[6].wait()


def scan_kernel(heads, first, got_ref, _, out_ref, flag_ref, *refs):
    flag_ref[...] = jnp.zeros_like(flag_ref)
    count = got_ref.shape[0]
    width = heads * HEAD
    seam = count - first

    def rolled(lanes):
        return jnp.concatenate([got_ref[seam:, 0, lanes], got_ref[:seam, 0, lanes]], axis=0)

    row, col = iota((CUT, width), 0), iota((CUT, width), 1)
    spread = jnp.where(row == col // HEAD * (CUT // heads), 1.0, 0.0)
    all_decays = sum_of_pieces(rolled(slice(width, width + CUT)), spread)
    groups = 8
    steps = count // groups
    for part in range(width // CUT):
        lanes = slice(part * CUT, (part + 1) * CUT)
        state_ref, decay_ref = refs[2 * part : 2 * part + 2]
        state_ref[...] = rolled(lanes)
        decay_ref[...] = all_decays[:, lanes]
        states, decays = [], []
        for j in range(steps):
            at = pl.ds(j, groups, stride=steps)
            state, decay = state_ref[at, :], decay_ref[at, :]
            if j:
                state, decay = state + decay * states[-1], decay * decays[-1]
            states.append(state)
            decays.append(decay)
        carries = [jnp.zeros((1, CUT), f32)]
        for g in range(groups - 1):
            carries.append(decays[-1][g : g + 1] * carries[-1] + states[-1][g : g + 1])
        carry = jnp.concatenate(carries, axis=0)
        for j in range(steps):
            before = states[j - 1] + decays[j - 1] * carry if j else carry
            state_ref[pl.ds(j, groups, stride=steps), :] = before
        out_ref[seam:, 0, lanes] = state_ref[:first, :]
        out_ref[:seam, 0, lanes] = state_ref[first:, :]


def early_kernel(
    skip_ref, x_ref, gate_ref, b_ref, c_ref, step_ref, keep_ref, base_ref, carry_ref, state_out, *scratch
):
    state_out[...] = cut_by_cut(
        0, skip_ref, x_ref, gate_ref, b_ref, c_ref, step_ref, keep_ref, base_ref, carry_ref,
        *scratch, jnp.zeros(state_out.shape, f32), lambda: None,
    )


def late_kernel(
    flag_ref, state_in, skip_ref, x_hbm, gate_hbm, b_hbm, c_hbm, step_hbm, keep_hbm,
    base_ref, carry_ref, *rest,
):
    *scratch, x_ref, gate_ref, b_ref, c_ref, step_ref, keep_ref, sems = rest
    size = x_ref.shape[0]
    mine = pl.ds(size, size)
    copies = [
        pltpu.make_async_copy(far, near, sems.at[i])
        for i, (far, near) in enumerate(
            (
                (keep_hbm, keep_ref),
                (step_hbm, step_ref),
                (c_hbm, c_ref),
                (b_hbm, b_ref),
                (x_hbm.at[mine], x_ref),
                (gate_hbm.at[mine], gate_ref),
            )
        )
    ]
    for copy in copies:
        copy.start()
    copies[0].wait()
    copies[1].wait()

    def wait_inputs():
        for copy in copies[2:]:
            copy.wait()

    cut_by_cut(
        size // CUT, skip_ref, x_ref, gate_ref, b_ref, c_ref, step_ref, keep_ref,
        base_ref, carry_ref, *scratch, state_in[...], wait_inputs,
    )


def cut_by_cut(
    skipped, skip_ref, x_ref, gate_ref, b_ref, c_ref, step_ref, keep_ref, base_ref, carry_ref,
    left, offset, factor, decays, starts, state, wait_inputs,
):
    heads, tokens = step_ref.shape
    cuts = tokens // CUT
    mine = x_ref.shape[0] // CUT
    count = heads * cuts
    step = by_cut(step_ref)
    row, col = iota((CUT, 3 * CUT), 0), iota((CUT, 3 * CUT), 1)
    kind = col // CUT
    kept = (kind == 2) | ((kind == 0) & (row <= col)) | ((kind == 1) & (row > col - CUT))
    sums = sum_of_pieces(by_cut(keep_ref), jnp.where(kept, 1.0, 0.0))
    upto, after, total = (sums[:, i * CUT : (i + 1) * CUT] for i in range(3))
    upto = upto * LOG2E
    row, col = iota((count, count), 0), iota((count, count), 1)
    earlier_cut = (row % heads == col % heads) & (col // heads < row // heads)
    factor[...] = jnp.exp(after) * step
    decays[...] = jnp.exp(total)
    starts[...] = jnp.exp(exact(jnp.where(earlier_cut, 1.0, 0.0), total))
    offset[...] = jnp.log2(jnp.maximum(step, 1e-37)) - upto
    for k in range(mine):
        rows = upto[(skipped + k) * heads : (skipped + k + 1) * heads]
        left[k] = jnp.concatenate([rows, jnp.zeros((8 - heads, CUT), f32)], axis=0)
    row, col = iota((CUT, CUT), 0), iota((CUT, CUT), 1)
    causal = row >= col
    low_lanes = jnp.where(iota((1, CUT), 1) < HEAD, 1.0, 0.0)
    only = [low_lanes.astype(bf16), (1.0 - low_lanes).astype(bf16)]

    def one_cut(k, now):
        at = pl.ds(pl.multiple_of(k * CUT, CUT), CUT)
        far = pl.ds(pl.multiple_of((skipped + k) * CUT, CUT), CUT)
        first = (skipped + k) * heads
        b = b_ref[:, far]
        c = jnp.transpose(c_ref[:, far])
        growths = jnp.transpose(left[k])
        growths = [jnp.broadcast_to(growths[:, h : h + 1], (CUT, CUT)) for h in range(heads)]
        scores = jnp.where(causal, dot(c, b), 0.0)
        b_turned = b.astype(f32)
        ends = []
        high = now.astype(bf16)
        low = (now - high.astype(f32)).astype(bf16)
        earlier = dot(jnp.concatenate([c, c], axis=1), jnp.concatenate([high, low], axis=0))
        for pair in range(heads // 2):
            lanes = slice(pair * CUT, (pair + 1) * CUT)
            x = x_ref[at, lanes]
            weights = []
            for h in range(2 * pair, 2 * pair + 2):
                gaps = growths[h] + offset[pl.ds(first + h, 1), :]
                weights.append((scores * jnp.exp2(jnp.minimum(gaps, 0.0))).astype(bf16))
            inside = dot(
                jnp.concatenate(weights, axis=1), jnp.concatenate([x * mask for mask in only], axis=0)
            )
            growth = jnp.exp2(two_heads(growths[2 * pair], growths[2 * pair + 1]))
            gate = gate_ref[at, lanes].astype(f32)
            gate = gate * pl.reciprocal(1.0 + jnp.exp(-gate))
            skip = two_heads(
                jnp.full((1, CUT), skip_ref[2 * pair]), jnp.full((1, CUT), skip_ref[2 * pair + 1])
            )
            base_ref[at, lanes] = (inside + growth * earlier[:, lanes] + skip * x.astype(f32)) * gate

            def per_channel(ref):
                even = first + 2 * pair
                return two_heads(ref[pl.ds(even, 1), :], ref[pl.ds(even + 1, 1), :])

            carry_ref[at, lanes] = (growth * per_channel(starts) * gate).astype(bf16)
            scaled = [b_turned * factor[pl.ds(first + 2 * pair + i, 1), :] for i in range(2)]
            both = dot(jnp.concatenate(scaled, axis=0).astype(bf16), x)
            ends.append(per_channel(decays) * now[:, lanes] + two_heads(both[:STATE], both[STATE:]))
        return jnp.concatenate(ends, axis=1)

    wait_inputs()
    return lax.fori_loop(0, mine, one_cut, state, unroll=UNROLL)


def gate_kernel(got_ref, c_ref, *refs):
    *parts, gated_ref, squares_ref = refs
    peers = squares_ref.shape[0]
    tokens = gated_ref.shape[0]
    now = got_ref[:, 0, :]
    high = now.astype(bf16)
    low = (now - high.astype(f32)).astype(bf16)
    both = jnp.concatenate([high, low], axis=0)
    ones = jnp.ones((8, 2 * CUT), bf16)
    size = 2 * CUT
    half_tokens = tokens // (len(parts) // 2)
    for k in range(tokens // size):
        at = slice(k * size, (k + 1) * size)
        c = c_ref[:, at]
        added = dot_tn(jnp.concatenate([c, c], axis=0), both)
        first = k * size
        base_ref, carry_ref = parts[2 * (first // half_tokens) : 2 * (first // half_tokens) + 2]
        here = slice(first % half_tokens, first % half_tokens + size)
        gated = base_ref[here, :] + carry_ref[here, :].astype(f32) * added
        gated_ref[at, :] = gated
        square = gated * gated
        square = square[:, :CUT] + square[:, CUT:]
        high = square.astype(bf16)
        low = (square - high.astype(f32)).astype(bf16)
        summed = dot_nt(ones, jnp.concatenate([high, low], axis=1))
        for peer in range(peers):
            for half in range(2):
                squares_ref[peer, 2 * k + half : 2 * k + half + 1, :] = summed[
                    :1, half * CUT : (half + 1) * CUT
                ]


def norm_kernel(got_ref, gain_ref, gated_ref, out_hbm, out_ref, sems):
    peers = got_ref.shape[0]
    cuts = got_ref.shape[1]
    summed = got_ref[0]
    for peer in range(1, peers):
        summed = summed + got_ref[peer]
    pieces = split3(lax.rsqrt(summed / CH + EPSILON))
    gain = gain_ref[...]
    ones = jnp.where(iota((8, gain.shape[1]), 0) < 3, 1.0, 0.0).astype(bf16)
    copies = []
    for k in range(cuts):
        at = slice(k * CUT, (k + 1) * CUT)
        rows = [piece[k : k + 1] for piece in pieces] + [jnp.zeros((5, CUT), f32)]
        factor = dot(jnp.transpose(jnp.concatenate(rows, axis=0)).astype(bf16), ones)
        out_ref[at, :] = (gated_ref[at, :] * factor * gain).astype(bf16)
        if k % 2 == 1:
            two = pl.ds((k - 1) * CUT, 2 * CUT)
            copy = pltpu.make_async_copy(out_ref.at[two], out_hbm.at[two], sems.at[k // 2])
            copy.start()
            copies.append(copy)
    for copy in copies:
        copy.wait()


VMEM = pl.BlockSpec(memory_space=pltpu.VMEM)
SMEM = pl.BlockSpec(memory_space=pltpu.SMEM)
HBM = pl.BlockSpec(memory_space=pltpu.HBM)


def call(kernel, out_shape, in_specs, scratch=(), out_specs=None, flops=1000000):
    return pl.pallas_call(
        kernel,
        out_shape=out_shape,
        in_specs=in_specs,
        out_specs=out_specs or jax.tree.map(lambda _: VMEM, out_shape),
        scratch_shapes=list(scratch),
        cost_estimate=pl.CostEstimate(flops=flops, bytes_accessed=4 * MIB, transcendentals=0),
        compiler_params=pltpu.CompilerParams(vmem_limit_bytes=16 * MIB),
    )


def exchange(v, axis):
    size, first = lax.axis_size(axis), FIRST[axis]
    places = [[(first + k) % size for k in range(size)]]
    return lax.all_to_all(v, axis, 0, 0, axis_index_groups=places, tiled=True)


def per_device(x_in, gate_in, b_in, c_in, step_size, log_keep, skip_gain, norm_gain):
    tokens, channels = x_in.shape
    heads = step_size.shape[0]
    cuts = tokens // CUT
    shape = jax.ShapeDtypeStruct
    dma = pltpu.SemaphoreType.DMA
    b_turned, c_turned = b_in.T, c_in.T
    x_in, gate_in, b_turned, c_far, step_size, log_keep, skip_gain = (
        pltpu.with_memory_space_constraint(v, pltpu.HBM)
        for v in (x_in, gate_in, b_turned, c_turned, step_size, log_keep, skip_gain)
    )
    rows = pltpu.VMEM((heads * cuts, CUT), f32)
    half = tokens // 2
    part = shape((half, channels), bf16)
    turned = shape((STATE, tokens), bf16)
    per_head = shape((heads, tokens), f32)
    near_shapes = (turned, turned, per_head, per_head)
    local_shapes = (shape((half, channels), f32), part)
    half_wide = pltpu.VMEM((half, channels), bf16)
    local_scratch = [pltpu.VMEM((cuts // 2, 8, CUT), f32), rows, rows, rows, rows]
    message, *near = call(
        end_state_kernel,
        (shape((STATE, 1, channels + CUT), f32), part, part, *near_shapes),
        [HBM] * 6,
        [half_wide, rows, dma((7,))],
        flops=2 * tokens * STATE * channels,
    )(x_in, gate_in, b_turned, c_far, step_size, log_keep)
    got = exchange(message, SEQ)
    base_0, carry_0, state = call(
        early_kernel,
        (*local_shapes, shape((STATE, channels), f32)),
        [SMEM] + [VMEM] * 6,
        local_scratch,
        flops=int(5e9),
    )(skip_gain, *near)
    before, flag = call(
        functools.partial(scan_kernel, heads, FIRST["seq"]),
        (shape((STATE, 1, channels), f32), shape((8, CUT), f32)),
        [VMEM] * 2,
        [pltpu.VMEM((STATE, CUT), f32)] * (2 * channels // CUT),
    )(got, state)
    entering = exchange(before, SEQ)
    base_1, carry_1 = call(
        late_kernel,
        local_shapes,
        [VMEM] * 2 + [SMEM] + [HBM] * 6,
        [
            *local_scratch, half_wide, half_wide,
            *(pltpu.VMEM(v.shape, v.dtype) for v in near_shapes), dma((6,)),
        ],
        flops=int(5e9),
    )(flag, state, skip_gain, x_in, gate_in, b_turned, c_far, step_size, log_keep)
    peers = lax.axis_size("chan")
    gated, squares = call(
        gate_kernel,
        (shape((tokens, channels), f32), shape((peers, cuts, CUT), f32)),
        [VMEM] * 6,
        flops=2 * tokens * STATE * channels,
    )(entering, c_turned, base_0, carry_0, base_1, carry_1)
    summed = exchange(squares, "chan")
    return call(
        norm_kernel,
        shape((tokens, channels), bf16),
        [VMEM] * 3,
        [pltpu.VMEM((tokens, channels), bf16), dma((cuts // 2,))],
        out_specs=HBM,
    )(summed, norm_gain.reshape(1, channels), gated)


def solution(mesh):
    placed = (
        P(SEQ, "chan"),
        P(SEQ, "chan"),
        P(SEQ, None),
        P(SEQ, None),
        P("chan", SEQ),
        P("chan", SEQ),
        P("chan"),
        P("chan"),
    )
    return jax.shard_map(
        per_device, mesh=mesh, in_specs=placed, out_specs=P(SEQ, "chan"), check_vma=False
    )
```

```python
import functools

import jax
import jax.numpy as jnp
from jax import lax
from jax.experimental import pallas as pl
from jax.experimental.pallas import tpu as pltpu
from jax.sharding import PartitionSpec as P

CH = 2048
HEAD = 64
STATE = 64
SEQ = "seq"
CUT = 128
EPSILON = 1e-05
LOG2E = 1.4426950408889634
MIB = 1024 * 1024
UNROLL = 4
FIRST = {"seq": 47, "chan": 5}

f32 = jnp.float32
bf16 = jnp.bfloat16


def dot(a, b):
    return jnp.dot(a, b, preferred_element_type=f32)


def dot_nt(a, b):
    return lax.dot_general(a, b, (((1,), (1,)), ((), ())), preferred_element_type=f32)


def dot_tn(a, b):
    return lax.dot_general(a, b, (((0,), (0,)), ((), ())), preferred_element_type=f32)


def iota(shape, axis):
    return lax.broadcasted_iota(jnp.int32, shape, axis)


def split3(v):
    high = v.astype(bf16).astype(f32)
    rest = v - high
    middle = rest.astype(bf16).astype(f32)
    return high, middle, rest - middle


def sum_of_pieces(v, zeros_and_ones):
    ones = zeros_and_ones.astype(bf16)
    high, middle, low = (dot(piece.astype(bf16), ones) for piece in split3(v))
    return high + (middle + low)


def by_cut(ref):
    tokens = ref.shape[1]
    return jnp.concatenate([ref[:, k * CUT : (k + 1) * CUT] for k in range(tokens // CUT)], axis=0)


def two_heads(even, odd):
    return jnp.where(iota(even.shape, 1) < HEAD, even, odd)


def end_state_kernel(
    x_hbm, gate_hbm, b_hbm, c_hbm, step_hbm, keep_hbm,
    out_ref, x_ref, gate_ref, b_ref, c_ref, step_ref, keep_ref,
    x_rest, factor, sems,
):
    half = x_ref.shape[0]
    copies = [
        pltpu.make_async_copy(source, target, sems.at[i])
        for i, (source, target) in enumerate(
            (
                (keep_hbm, keep_ref),
                (step_hbm, step_ref),
                (b_hbm, b_ref),
                (x_hbm.at[pl.ds(0, half)], x_ref),
                (x_hbm.at[pl.ds(half, half)], x_rest),
                (c_hbm, c_ref),
                (gate_hbm.at[pl.ds(0, half)], gate_ref),
            )
        )
    ]
    for copy in copies:
        copy.start()
    heads, tokens = step_ref.shape
    cuts = tokens // CUT
    row, col = iota((CUT, 2 * CUT), 0), iota((CUT, 2 * CUT), 1)
    kept = jnp.where((row > col) | (col >= CUT), 1.0, 0.0)
    copies[0].wait()
    sums = sum_of_pieces(by_cut(keep_ref), kept)
    after, total = sums[:, :CUT], sums[:, CUT:]
    count = heads * cuts
    row, col = iota((count, count), 0), iota((count, count), 1)
    same = row % heads == col % heads
    mask = jnp.where(same & (col // heads > row // heads), 1.0, 0.0).astype(bf16)
    later = sum(dot(mask, piece.astype(bf16)) for piece in reversed(split3(total)))
    decay = jnp.exp(later[:heads] + total[:heads])
    lane = iota((1, CUT), 1) // (CUT // heads)
    decays = jnp.zeros((1, CUT), f32)
    for h in range(heads):
        decays = jnp.where(lane == h, decay[h : h + 1], decays)
    copies[1].wait()
    factor[...] = jnp.exp(after + later) * by_cut(step_ref)
    copies[2].wait()
    pairs = heads // 2
    both = [jnp.zeros((2 * STATE, CUT), f32)] * pairs
    for k in range(0, cuts, 2):
        at = k * CUT
        near = x_ref if at < half else x_rest
        if at % half == 0:
            copies[3 + at // half].wait()
        part = b_ref[:, at : at + 2 * CUT].astype(f32)
        for pair in range(pairs):
            lhs = []
            for h in range(2 * pair, 2 * pair + 2):
                rows = [factor[(k + i) * heads + h : (k + i) * heads + h + 1, :] for i in range(2)]
                lhs.append((part * jnp.concatenate(rows, axis=1)).astype(bf16))
            x = near[at % half : at % half + 2 * CUT, pair * CUT : (pair + 1) * CUT]
            both[pair] = both[pair] + dot(jnp.concatenate(lhs, axis=0), x)
    for pair in range(pairs):
        lanes = slice(pair * CUT, (pair + 1) * CUT)
        out_ref[:, 0, lanes] = two_heads(both[pair][:STATE], both[pair][STATE:])
    out_ref[:, 0, pairs * CUT :] = jnp.broadcast_to(decays, (STATE, CUT))
    copies[5].wait()
    copies[6].wait()


def scan_kernel(heads, first, got_ref, _, out_ref, flag_ref, *refs):
    flag_ref[...] = jnp.zeros_like(flag_ref)
    count = got_ref.shape[0]
    width = heads * HEAD
    seam = count - first

    def rolled(lanes):
        return jnp.concatenate([got_ref[seam:, 0, lanes], got_ref[:seam, 0, lanes]], axis=0)

    row, col = iota((CUT, width), 0), iota((CUT, width), 1)
    spread = jnp.where(row == col // HEAD * (CUT // heads), 1.0, 0.0)
    all_decays = sum_of_pieces(rolled(slice(width, width + CUT)), spread)
    groups = 8
    steps = count // groups
    for part in range(width // CUT):
        lanes = slice(part * CUT, (part + 1) * CUT)
        state_ref, decay_ref = refs[2 * part : 2 * part + 2]
        state_ref[...] = rolled(lanes)
        decay_ref[...] = all_decays[:, lanes]
        states, decays = [], []
        for j in range(steps):
            at = pl.ds(j, groups, stride=steps)
            state, decay = state_ref[at, :], decay_ref[at, :]
            if j:
                state, decay = state + decay * states[-1], decay * decays[-1]
            states.append(state)
            decays.append(decay)
        carries = [jnp.zeros((1, CUT), f32)]
        for g in range(groups - 1):
            carries.append(decays[-1][g : g + 1] * carries[-1] + states[-1][g : g + 1])
        carry = jnp.concatenate(carries, axis=0)
        for j in range(steps):
            before = states[j - 1] + decays[j - 1] * carry if j else carry
            state_ref[pl.ds(j, groups, stride=steps), :] = before
        out_ref[seam:, 0, lanes] = state_ref[:first, :]
        out_ref[:seam, 0, lanes] = state_ref[first:, :]


def early_kernel(
    skip_ref, x_ref, gate_ref, b_ref, c_ref, step_ref, keep_ref, base_ref, carry_ref, state_out, *scratch
):
    state_out[...] = cut_by_cut(
        0, skip_ref, x_ref, gate_ref, b_ref, c_ref, step_ref, keep_ref, base_ref, carry_ref,
        *scratch, jnp.zeros(state_out.shape, f32), lambda: None,
    )


def late_kernel(
    flag_ref, state_in, skip_ref, x_hbm, gate_hbm, b_hbm, c_hbm, step_hbm, keep_hbm,
    base_ref, carry_ref, *rest,
):
    *scratch, x_ref, gate_ref, b_ref, c_ref, step_ref, keep_ref, sems = rest
    size = x_ref.shape[0]
    mine = pl.ds(size, size)
    copies = [
        pltpu.make_async_copy(far, near, sems.at[i])
        for i, (far, near) in enumerate(
            (
                (keep_hbm, keep_ref),
                (step_hbm, step_ref),
                (x_hbm.at[mine], x_ref),
                (gate_hbm.at[mine], gate_ref),
                (b_hbm.at[:, mine], b_ref.at[:, mine]),
                (c_hbm.at[:, mine], c_ref.at[:, mine]),
            )
        )
    ]
    for copy in copies:
        copy.start()
    copies[0].wait()
    copies[1].wait()

    def wait_inputs():
        for copy in copies[2:]:
            copy.wait()

    cut_by_cut(
        size // CUT, skip_ref, x_ref, gate_ref, b_ref, c_ref, step_ref, keep_ref,
        base_ref, carry_ref, *scratch, state_in[...], wait_inputs,
    )


def cut_by_cut(
    skipped, skip_ref, x_ref, gate_ref, b_ref, c_ref, step_ref, keep_ref, base_ref, carry_ref,
    left, offset, factor, decays, starts, state, wait_inputs,
):
    heads, tokens = step_ref.shape
    cuts = tokens // CUT
    mine = x_ref.shape[0] // CUT
    count = heads * cuts
    step = by_cut(step_ref)
    row, col = iota((CUT, 3 * CUT), 0), iota((CUT, 3 * CUT), 1)
    kind = col // CUT
    kept = (kind == 2) | ((kind == 0) & (row <= col)) | ((kind == 1) & (row > col - CUT))
    sums = sum_of_pieces(by_cut(keep_ref), jnp.where(kept, 1.0, 0.0))
    upto, after, total = (sums[:, i * CUT : (i + 1) * CUT] for i in range(3))
    upto = upto * LOG2E
    row, col = iota((count, count), 0), iota((count, count), 1)
    earlier_cut = (row % heads == col % heads) & (col // heads < row // heads)
    factor[...] = jnp.exp(after) * step
    decays[...] = jnp.exp(total)
    mask = jnp.where(earlier_cut, 1.0, 0.0).astype(bf16)
    before = sum(dot(mask, piece.astype(bf16)) for piece in reversed(split3(total)))
    starts[...] = jnp.exp(before)
    offset[...] = jnp.log2(jnp.maximum(step, 1e-37)) - upto
    for k in range(mine):
        rows = upto[(skipped + k) * heads : (skipped + k + 1) * heads]
        left[k] = jnp.concatenate([rows, jnp.zeros((8 - heads, CUT), f32)], axis=0)
    row, col = iota((CUT, CUT), 0), iota((CUT, CUT), 1)
    causal = row >= col
    low_lanes = jnp.where(iota((1, CUT), 1) < HEAD, 1.0, 0.0)
    only = [low_lanes.astype(bf16), (1.0 - low_lanes).astype(bf16)]

    def one_cut(k, now):
        at = pl.ds(pl.multiple_of(k * CUT, CUT), CUT)
        far = pl.ds(pl.multiple_of((skipped + k) * CUT, CUT), CUT)
        first = (skipped + k) * heads
        b = b_ref[:, far]
        c = jnp.transpose(c_ref[:, far])
        growths = jnp.transpose(left[k])
        growths = [jnp.broadcast_to(growths[:, h : h + 1], (CUT, CUT)) for h in range(heads)]
        scores = jnp.where(causal, dot(c, b), 0.0)
        b_turned = b.astype(f32)
        ends = []
        high = now.astype(bf16)
        low = (now - high.astype(f32)).astype(bf16)
        earlier = dot(jnp.concatenate([c, c], axis=1), jnp.concatenate([high, low], axis=0))
        for pair in range(heads // 2):
            lanes = slice(pair * CUT, (pair + 1) * CUT)
            x = x_ref[at, lanes]
            weights = []
            for h in range(2 * pair, 2 * pair + 2):
                gaps = growths[h] + offset[pl.ds(first + h, 1), :]
                weights.append((scores * jnp.exp2(jnp.minimum(gaps, 0.0))).astype(bf16))
            inside = dot(
                jnp.concatenate(weights, axis=1), jnp.concatenate([x * mask for mask in only], axis=0)
            )
            growth = jnp.exp2(two_heads(growths[2 * pair], growths[2 * pair + 1]))
            gate = gate_ref[at, lanes].astype(f32)
            gate = gate * pl.reciprocal(1.0 + jnp.exp(-gate))
            skip = two_heads(
                jnp.full((1, CUT), skip_ref[2 * pair]), jnp.full((1, CUT), skip_ref[2 * pair + 1])
            )
            base_ref[at, lanes] = (inside + growth * earlier[:, lanes] + skip * x.astype(f32)) * gate

            def per_channel(ref):
                even = first + 2 * pair
                return two_heads(ref[pl.ds(even, 1), :], ref[pl.ds(even + 1, 1), :])

            carry_ref[at, lanes] = (growth * per_channel(starts) * gate).astype(bf16)
            scaled = [b_turned * factor[pl.ds(first + 2 * pair + i, 1), :] for i in range(2)]
            both = dot(jnp.concatenate(scaled, axis=0).astype(bf16), x)
            ends.append(per_channel(decays) * now[:, lanes] + two_heads(both[:STATE], both[STATE:]))
        return jnp.concatenate(ends, axis=1)

    wait_inputs()
    return lax.fori_loop(0, mine, one_cut, state, unroll=UNROLL)


def gate_kernel(got_ref, c_ref, *refs):
    *parts, gated_ref, squares_ref = refs
    peers = squares_ref.shape[0]
    tokens = gated_ref.shape[0]
    now = got_ref[:, 0, :]
    high = now.astype(bf16)
    low = (now - high.astype(f32)).astype(bf16)
    both = jnp.concatenate([high, low], axis=0)
    ones = jnp.ones((8, 2 * CUT), bf16)
    size = 2 * CUT
    half_tokens = tokens // (len(parts) // 2)
    for k in range(tokens // size):
        at = slice(k * size, (k + 1) * size)
        c = c_ref[:, at]
        added = dot_tn(jnp.concatenate([c, c], axis=0), both)
        first = k * size
        base_ref, carry_ref = parts[2 * (first // half_tokens) : 2 * (first // half_tokens) + 2]
        here = slice(first % half_tokens, first % half_tokens + size)
        gated = base_ref[here, :] + carry_ref[here, :].astype(f32) * added
        gated_ref[at, :] = gated
        square = gated * gated
        square = square[:, :CUT] + square[:, CUT:]
        high = square.astype(bf16)
        low = (square - high.astype(f32)).astype(bf16)
        summed = dot_nt(ones, jnp.concatenate([high, low], axis=1))
        for peer in range(peers):
            for half in range(2):
                squares_ref[peer, 2 * k + half : 2 * k + half + 1, :] = summed[
                    :1, half * CUT : (half + 1) * CUT
                ]


def norm_kernel(got_ref, gain_ref, gated_ref, out_hbm, out_ref, sems):
    peers = got_ref.shape[0]
    cuts = got_ref.shape[1]
    summed = got_ref[0]
    for peer in range(1, peers):
        summed = summed + got_ref[peer]
    pieces = split3(lax.rsqrt(summed / CH + EPSILON))
    gain = gain_ref[...]
    ones = jnp.where(iota((8, gain.shape[1]), 0) < 3, 1.0, 0.0).astype(bf16)
    copies = []
    for k in range(cuts):
        at = slice(k * CUT, (k + 1) * CUT)
        rows = [piece[k : k + 1] for piece in pieces] + [jnp.zeros((5, CUT), f32)]
        factor = dot(jnp.transpose(jnp.concatenate(rows, axis=0)).astype(bf16), ones)
        out_ref[at, :] = (gated_ref[at, :] * factor * gain).astype(bf16)
        if k % 2 == 1:
            two = pl.ds((k - 1) * CUT, 2 * CUT)
            copy = pltpu.make_async_copy(out_ref.at[two], out_hbm.at[two], sems.at[k // 2])
            copy.start()
            copies.append(copy)
    for copy in copies:
        copy.wait()


VMEM = pl.BlockSpec(memory_space=pltpu.VMEM)
SMEM = pl.BlockSpec(memory_space=pltpu.SMEM)
HBM = pl.BlockSpec(memory_space=pltpu.HBM)


def call(kernel, out_shape, in_specs, scratch=(), out_specs=None, flops=1000000):
    return pl.pallas_call(
        kernel,
        out_shape=out_shape,
        in_specs=in_specs,
        out_specs=out_specs or jax.tree.map(lambda _: VMEM, out_shape),
        scratch_shapes=list(scratch),
        cost_estimate=pl.CostEstimate(flops=flops, bytes_accessed=4 * MIB, transcendentals=0),
        compiler_params=pltpu.CompilerParams(vmem_limit_bytes=16 * MIB),
    )


def exchange(v, axis):
    size, first = lax.axis_size(axis), FIRST[axis]
    places = [[(first + k) % size for k in range(size)]]
    return lax.all_to_all(v, axis, 0, 0, axis_index_groups=places, tiled=True)


def per_device(x_in, gate_in, b_in, c_in, step_size, log_keep, skip_gain, norm_gain):
    tokens, channels = x_in.shape
    heads = step_size.shape[0]
    cuts = tokens // CUT
    shape = jax.ShapeDtypeStruct
    dma = pltpu.SemaphoreType.DMA
    b_turned, c_turned = b_in.T, c_in.T
    x_in, gate_in, b_turned, c_far, step_size, log_keep, skip_gain = (
        pltpu.with_memory_space_constraint(v, pltpu.HBM)
        for v in (x_in, gate_in, b_turned, c_turned, step_size, log_keep, skip_gain)
    )
    rows = pltpu.VMEM((heads * cuts, CUT), f32)
    half = tokens // 2
    part = shape((half, channels), bf16)
    turned = shape((STATE, tokens), bf16)
    per_head = shape((heads, tokens), f32)
    near_shapes = (turned, turned, per_head, per_head)
    local_shapes = (shape((half, channels), f32), part)
    half_wide = pltpu.VMEM((half, channels), bf16)
    local_scratch = [pltpu.VMEM((cuts // 2, 8, CUT), f32), rows, rows, rows, rows]
    message, *near = call(
        end_state_kernel,
        (shape((STATE, 1, channels + CUT), f32), part, part, *near_shapes),
        [HBM] * 6,
        [half_wide, rows, dma((7,))],
        flops=2 * tokens * STATE * channels,
    )(x_in, gate_in, b_turned, c_far, step_size, log_keep)
    got = exchange(message, SEQ)
    base_0, carry_0, state = call(
        early_kernel,
        (*local_shapes, shape((STATE, channels), f32)),
        [SMEM] + [VMEM] * 6,
        local_scratch,
        flops=int(5e9),
    )(skip_gain, *near)
    before, flag = call(
        functools.partial(scan_kernel, heads, FIRST["seq"]),
        (shape((STATE, 1, channels), f32), shape((8, CUT), f32)),
        [VMEM] * 2,
        [pltpu.VMEM((STATE, CUT), f32)] * (2 * channels // CUT),
    )(got, state)
    entering = exchange(before, SEQ)
    base_1, carry_1 = call(
        late_kernel,
        local_shapes,
        [VMEM] * 2 + [SMEM] + [HBM] * 6,
        [
            *local_scratch, half_wide, half_wide,
            *(pltpu.VMEM(v.shape, v.dtype) for v in near_shapes), dma((6,)),
        ],
        flops=int(5e9),
    )(flag, state, skip_gain, x_in, gate_in, b_turned, c_far, step_size, log_keep)
    peers = lax.axis_size("chan")
    gated, squares = call(
        gate_kernel,
        (shape((tokens, channels), f32), shape((peers, cuts, CUT), f32)),
        [VMEM] * 6,
        flops=2 * tokens * STATE * channels,
    )(entering, c_turned, base_0, carry_0, base_1, carry_1)
    summed = exchange(squares, "chan")
    return call(
        norm_kernel,
        shape((tokens, channels), bf16),
        [VMEM] * 3,
        [pltpu.VMEM((tokens, channels), bf16), dma((cuts // 2,))],
        out_specs=HBM,
    )(summed, norm_gain.reshape(1, channels), gated)


def solution(mesh):
    placed = (
        P(SEQ, "chan"),
        P(SEQ, "chan"),
        P(SEQ, None),
        P(SEQ, None),
        P("chan", SEQ),
        P("chan", SEQ),
        P("chan"),
        P("chan"),
    )
    return jax.shard_map(
        per_device, mesh=mesh, in_specs=placed, out_specs=P(SEQ, "chan"), check_vma=False
    )
```
